32 devices in a mesh: dp: 8 (over y, x, core), tensor: 4 (over z).
Axes of the slice: x: 2, y: 2, z: 4, core: 2. Of those that a mesh axis runs over, the one named last changes fastest.
Arguments:
- tokens: bfloat16 [4096, 2304], P(('dp', 'tensor')), may hold values from -6 to 6
- cotangent: bfloat16 [4096, 4096], P('dp', 'tensor'), may hold values from -6 to 6
- pre_gain: float32 [2304], replicated, may hold values from 0.25 to 1.75
- w_query: bfloat16 [2304, 4096], P('dp', 'tensor'), may hold values from -0.375 to 0.375
- key_weight: bfloat16 [2304, 2048], P('dp', 'tensor'), may hold values from -0.375 to 0.375
- value_weight: bfloat16 [2304, 2048], P('dp', 'tensor'), may hold values from -0.125 to 0.125
Outputs:
- attended: bfloat16 [4096, 4096], P('dp', 'tensor')
- grad_tokens: bfloat16 [4096, 2304], P(('dp', 'tensor'))
- grad_query: float32 [2304, 4096], P('dp', 'tensor')
- grad_key: float32 [2304, 2048], P('dp', 'tensor')
- grad_value: float32 [2304, 2048], P('dp', 'tensor')
- grad_pre_gain: float32 [2304], replicated
The draws below stay inside these ranges and needn't reach their ends.
All inputs are finite; a program needn't handle non-finite values.
Results may differ from the reference program's by a relative error of at most 0.019.
The reference program's roundings to bfloat16 on the way count: a program that leaves them out, or rounds other values in their place, can miss the bound.
Values may be sent and summed in bfloat16 or wider, within the bound.
A program may use at most 192 MiB of HBM per device.

```python
import jax
import jax.numpy as jnp
from jax import lax

MODEL_WIDTH = 2304
QUERY_HEADS = 32
KEY_VALUE_HEADS = 16
HEAD_SIZE = 128
TOK_DEV = 128
SEQ_LEN = 64
TOKENS = 4096
N_DP = 8
N_TENSOR = 4


def block_levels(own_key, dims, cuts, least, high):
    level = 1.0
    for dim, parts in cuts:
        heights = jax.random.uniform(jax.random.fold_in(jax.random.fold_in(own_key, 6), dim), (parts,), jnp.float32, least / len(cuts), high / len(cuts))
        level = level * jnp.repeat(jnp.exp(heights), dims[dim] // parts).reshape((-1,) + (1,) * (len(dims) - 1 - dim))
    return level


def bell_draw(rng, shape, spread, reach, cuts=(), kind=jnp.bfloat16):
    factor_of = block_levels(rng, shape, cuts, -0.22, 0.18) if cuts else 1.0
    result = jax.random.normal(rng, shape, jnp.float32) * spread * factor_of
    return jnp.minimum(jnp.maximum(result, -reach), reach).astype(kind)


def setup_inputs(seed: int = 0) -> dict:
    key_list = jax.random.split(jax.random.key(seed), 7)
    tokens = bell_draw(key_list[0], (TOKENS, MODEL_WIDTH), 1.0, 6.0, ((0, 32),))
    cotangent = bell_draw(key_list[1], (TOKENS, QUERY_HEADS * HEAD_SIZE), 1.0, 6.0, ((0, 8), (1, 4)))
    pre_gain = jnp.clip(1.0 + 0.15 * jax.random.normal(key_list[2], (MODEL_WIDTH,), jnp.float32), 0.25, 1.75)
    w_query = bell_draw(key_list[3], (MODEL_WIDTH, QUERY_HEADS * HEAD_SIZE), (MODEL_WIDTH // 9) ** -0.5, 0.375, ((0, 8), (1, 4)))
    key_weight = bell_draw(key_list[4], (MODEL_WIDTH, KEY_VALUE_HEADS * HEAD_SIZE), (MODEL_WIDTH // 9) ** -0.5, 0.375, ((0, 8), (1, 4)))
    value_weight = bell_draw(key_list[5], (MODEL_WIDTH, KEY_VALUE_HEADS * HEAD_SIZE), MODEL_WIDTH ** -0.5, 0.125, ((0, 8), (1, 4)))
    return {"tokens": tokens, "cotangent": cotangent, "pre_gain": pre_gain, "w_query": w_query, "key_weight": key_weight, "value_weight": value_weight}


EPS = 1e-06
CAP = 50.0
BASE = 10000.0
query_scalar = 144.0

def rotary_tables(segment_length, half):
    places = jnp.arange(segment_length, dtype=jnp.float32)[:, None]
    freqs = BASE ** (-jnp.arange(half, dtype=jnp.float32) / half)
    angles = places * freqs[None, :]
    return (jnp.cos(angles)[:, None, :], jnp.sin(angles)[:, None, :])

def rotate(values, cosine_table, sine_table):
    half = values.shape[-1] // 2
    first, second = (values[..., :half], values[..., half:])
    return jnp.concatenate([first * cosine_table - second * sine_table, second * cosine_table + first * sine_table], -1)

def inverse_rotation(values, cosine_table, sine_table):
    half = values.shape[-1] // 2
    first, second = (values[..., :half], values[..., half:])
    return jnp.concatenate([first * cosine_table + second * sine_table, second * cosine_table - first * sine_table], -1)

def attend_forward(query, key, value):
    repeat = query.shape[1] // key.shape[1]
    keys = jnp.repeat(key, repeat, axis=1).astype(jnp.float32)
    values = jnp.repeat(value, repeat, axis=1).astype(jnp.float32)
    factor = query_scalar ** (-0.5)
    raw = jnp.einsum('qhd,khd->hqk', query.astype(jnp.float32), keys) * factor
    bent = jnp.tanh(raw / CAP)
    capped = CAP * bent
    segment_length = query.shape[0]
    causal = jnp.arange(segment_length)[None, :] <= jnp.arange(segment_length)[:, None]
    raised = jnp.where(causal[None], jnp.exp(capped), 0.0)
    weights = raised / lax.optimization_barrier(jnp.sum(raised, -1, keepdims=True))
    probs = weights.astype(jnp.bfloat16)
    attended = jnp.einsum('hqk,khd->qhd', probs.astype(jnp.float32), values).astype(jnp.bfloat16)
    return (attended, weights, probs, bent)

def attend_backward(d_attended, query, key, value, weights, probs, bent):
    repeat = query.shape[1] // key.shape[1]
    keys = jnp.repeat(key, repeat, axis=1).astype(jnp.float32)
    values = jnp.repeat(value, repeat, axis=1).astype(jnp.float32)
    factor = query_scalar ** (-0.5)
    grad_in = d_attended.astype(jnp.float32)
    d_probs = jnp.einsum('qhd,khd->hqk', grad_in, values)
    d_capped = weights * (d_probs - lax.optimization_barrier(jnp.sum(weights * d_probs, -1, keepdims=True)))
    d_scores = (d_capped * (1.0 - bent * bent) * factor).astype(jnp.bfloat16).astype(jnp.float32)
    query_back = jnp.einsum('hqk,khd->qhd', d_scores, keys)
    key_heads = jnp.einsum('hqk,qhd->khd', d_scores, query.astype(jnp.float32))
    value_heads = jnp.einsum('hqk,qhd->khd', probs.astype(jnp.float32), grad_in)
    segment_length, heads, width = query.shape
    key_rotated_back = key_heads.reshape(segment_length, heads // repeat, repeat, width).sum(2)
    value_returned = value_heads.reshape(segment_length, heads // repeat, repeat, width).sum(2)
    return (query_back, key_rotated_back, value_returned)

def reference(tokens, cotangent, pre_gain, w_query, key_weight, value_weight):
    segment_length = TOK_DEV * N_TENSOR
    token_span = SEQ_LEN
    pieces_count = segment_length // token_span
    query_groups = N_TENSOR
    col_query = QUERY_HEADS * HEAD_SIZE // query_groups
    column_key = KEY_VALUE_HEADS * HEAD_SIZE // query_groups
    cosine_table, sine_table = rotary_tables(token_span, HEAD_SIZE // 2)

    def one_block(carry, pieces):
        rows, cot_rows = pieces
        rows_f = rows.astype(jnp.float32)
        inv_one = lax.rsqrt(lax.optimization_barrier(jnp.mean(rows_f * rows_f, -1, keepdims=True)) + EPS)
        unit_one = rows_f * inv_one
        normed_input = (unit_one * pre_gain).astype(jnp.bfloat16)
        query_raw = jnp.dot(normed_input, w_query, preferred_element_type=jnp.float32).reshape(pieces_count, token_span, QUERY_HEADS, HEAD_SIZE)
        key_unrotated = jnp.dot(normed_input, key_weight, preferred_element_type=jnp.float32).reshape(pieces_count, token_span, KEY_VALUE_HEADS, HEAD_SIZE)
        value_projected = jnp.dot(normed_input, value_weight, preferred_element_type=jnp.float32).reshape(pieces_count, token_span, KEY_VALUE_HEADS, HEAD_SIZE)
        query = rotate(query_raw, cosine_table, sine_table).astype(jnp.bfloat16)
        key = rotate(key_unrotated, cosine_table, sine_table).astype(jnp.bfloat16)
        value = value_projected.astype(jnp.bfloat16)
        attended, weights, probs, bent = jax.vmap(attend_forward)(query, key, value)
        attended = attended.reshape(segment_length, QUERY_HEADS * HEAD_SIZE)
        d_attended = cot_rows.reshape(pieces_count, token_span, QUERY_HEADS, HEAD_SIZE)
        query_back, key_rotated_back, value_returned = jax.vmap(attend_backward)(d_attended, query, key, value, weights, probs, bent)
        d_query = inverse_rotation(query_back, cosine_table, sine_table).astype(jnp.bfloat16).reshape(segment_length, QUERY_HEADS * HEAD_SIZE)
        key_gradient = inverse_rotation(key_rotated_back, cosine_table, sine_table).astype(jnp.bfloat16).reshape(segment_length, KEY_VALUE_HEADS * HEAD_SIZE)
        value_gradient = value_returned.astype(jnp.bfloat16).reshape(segment_length, KEY_VALUE_HEADS * HEAD_SIZE)
        query_part = jnp.dot(normed_input.T, d_query, preferred_element_type=jnp.float32)
        key_part = jnp.dot(normed_input.T, key_gradient, preferred_element_type=jnp.float32)
        value_part = jnp.dot(normed_input.T, value_gradient, preferred_element_type=jnp.float32)
        back = jnp.einsum('lgc,dgc->lgd', d_query.reshape(segment_length, query_groups, col_query).astype(jnp.float32), w_query.reshape(MODEL_WIDTH, query_groups, col_query).astype(jnp.float32))
        back = back + jnp.einsum('lgc,dgc->lgd', key_gradient.reshape(segment_length, query_groups, column_key).astype(jnp.float32), key_weight.reshape(MODEL_WIDTH, query_groups, column_key).astype(jnp.float32))
        back = back + jnp.einsum('lgc,dgc->lgd', value_gradient.reshape(segment_length, query_groups, column_key).astype(jnp.float32), value_weight.reshape(MODEL_WIDTH, query_groups, column_key).astype(jnp.float32))
        back = lax.optimization_barrier(back.astype(jnp.bfloat16))
        d_normed = lax.optimization_barrier(jnp.sum(back.astype(jnp.float32), 1))
        pre_part = lax.optimization_barrier(jnp.sum(d_normed * unit_one, 0))
        scaled_in = d_normed * pre_gain
        grad_rows = (inv_one * (scaled_in - unit_one * lax.optimization_barrier(jnp.mean(scaled_in * unit_one, -1, keepdims=True)))).astype(jnp.bfloat16)
        rounded = lax.optimization_barrier(tuple((part.astype(jnp.bfloat16) for part in (query_part, key_part, value_part))))
        sums = tuple((total + part.astype(jnp.float32) for total, part in zip(carry[:3], rounded)))
        carry = sums + (carry[3] + pre_part,)
        return (carry, (attended, grad_rows))
    start_offset = (jnp.zeros((MODEL_WIDTH, QUERY_HEADS * HEAD_SIZE), jnp.float32), jnp.zeros((MODEL_WIDTH, KEY_VALUE_HEADS * HEAD_SIZE), jnp.float32), jnp.zeros((MODEL_WIDTH, KEY_VALUE_HEADS * HEAD_SIZE), jnp.float32), jnp.zeros((MODEL_WIDTH,), jnp.float32))
    pieces = (tokens.reshape(N_DP, segment_length, MODEL_WIDTH), cotangent.reshape(N_DP, segment_length, QUERY_HEADS * HEAD_SIZE))
    totals, (attended, grad_tokens) = lax.scan(one_block, start_offset, pieces)
    return (attended.reshape(N_DP * segment_length, QUERY_HEADS * HEAD_SIZE), grad_tokens.reshape(N_DP * segment_length, MODEL_WIDTH), totals[0], totals[1], totals[2], totals[3])
```

```python
import functools

import jax
import jax.numpy as jnp
import numpy as np
from jax import lax
from jax.experimental import pallas as pl
from jax.experimental.pallas import tpu as pltpu
from jax.sharding import PartitionSpec as P

HEAD_SIZE = 128
SEQ_LEN = 64


EPS = 1e-06
CAP = 50.0
BASE = 10000.0
query_scalar = 144.0


def rotary_tables(segment_length, half):
    places = jnp.arange(segment_length, dtype=jnp.float32)[:, None]
    freqs = BASE ** (-jnp.arange(half, dtype=jnp.float32) / half)
    angles = places * freqs[None, :]
    return (jnp.cos(angles)[:, None, :], jnp.sin(angles)[:, None, :])


def rotate(values, cosine_table, sine_table):
    half = values.shape[-1] // 2
    first, second = (values[..., :half], values[..., half:])
    return jnp.concatenate(
        [first * cosine_table - second * sine_table, second * cosine_table + first * sine_table], -1
    )


def inverse_rotation(values, cosine_table, sine_table):
    half = values.shape[-1] // 2
    first, second = (values[..., :half], values[..., half:])
    return jnp.concatenate(
        [first * cosine_table + second * sine_table, second * cosine_table - first * sine_table], -1
    )


def attend_forward(query, key, value):
    repeat = query.shape[1] // key.shape[1]
    keys = jnp.repeat(key, repeat, axis=1)
    values = jnp.repeat(value, repeat, axis=1)
    factor = query_scalar ** (-0.5)
    raw = jnp.einsum("qhd,khd->hqk", query, keys, preferred_element_type=jnp.float32) * factor
    bent = jnp.tanh(raw / CAP)
    capped = CAP * bent
    segment_length = query.shape[0]
    causal = jnp.arange(segment_length)[None, :] <= jnp.arange(segment_length)[:, None]
    raised = jnp.where(causal[None], jnp.exp(capped), 0.0)
    weights = raised / jnp.sum(raised, -1, keepdims=True)
    probs = weights.astype(jnp.bfloat16)
    attended = jnp.einsum("hqk,khd->qhd", probs, values, preferred_element_type=jnp.float32).astype(
        jnp.bfloat16
    )
    return (attended, weights, probs, bent)


def attend_backward(d_attended, query, key, value, weights, probs, bent):
    repeat = query.shape[1] // key.shape[1]
    keys = jnp.repeat(key, repeat, axis=1)
    values = jnp.repeat(value, repeat, axis=1)
    factor = query_scalar ** (-0.5)
    d_probs = jnp.einsum("qhd,khd->hqk", d_attended, values, preferred_element_type=jnp.float32)
    d_capped = weights * (d_probs - jnp.sum(weights * d_probs, -1, keepdims=True))
    d_scores = (d_capped * (1.0 - bent * bent) * factor).astype(jnp.bfloat16)
    query_back = jnp.einsum("hqk,khd->qhd", d_scores, keys, preferred_element_type=jnp.float32)
    key_heads = jnp.einsum("hqk,qhd->khd", d_scores, query, preferred_element_type=jnp.float32)
    value_heads = jnp.einsum("hqk,qhd->khd", probs, d_attended, preferred_element_type=jnp.float32)
    segment_length, heads, width = query.shape
    key_rotated_back = key_heads.reshape(segment_length, heads // repeat, repeat, width).sum(2)
    value_returned = value_heads.reshape(segment_length, heads // repeat, repeat, width).sum(2)
    return (query_back, key_rotated_back, value_returned)


def segment_pass(query, key, value, d_attended):
    attended, weights, probs, bent = attend_forward(query, key, value)
    query_back, key_rotated_back, value_returned = attend_backward(
        d_attended, query, key, value, weights, probs, bent
    )
    return (attended, query_back, key_rotated_back, value_returned)


def per_device(tokens, cotangent, pre_gain, w_query, key_weight, value_weight):
    contract_first = (((0,), (0,)), ((), ()))
    contract_last = (((1,), (1,)), ((), ()))
    rows_f = tokens.astype(jnp.float32)
    inv_one = lax.rsqrt(jnp.mean(rows_f * rows_f, -1, keepdims=True) + EPS)
    unit_one = rows_f * inv_one
    normed_input = (unit_one * pre_gain).astype(jnp.bfloat16)
    gathered = lax.all_gather(normed_input, "tensor", axis=0, tiled=True)
    segment_length = gathered.shape[0]
    token_span = SEQ_LEN
    pieces_count = segment_length // token_span
    heads_query = w_query.shape[1] // HEAD_SIZE
    heads_key = key_weight.shape[1] // HEAD_SIZE
    pieces = (
        lax.all_gather(w_query, "dp", axis=0, tiled=True),
        lax.all_gather(key_weight, "dp", axis=0, tiled=True),
        lax.all_gather(value_weight, "dp", axis=0, tiled=True),
    )
    query_raw, key_unrotated, value_projected = tuple(
        (jnp.dot(gathered, piece, preferred_element_type=jnp.float32) for piece in pieces)
    )
    cosine_table, sine_table = rotary_tables(token_span, HEAD_SIZE // 2)
    query = rotate(
        query_raw.reshape(pieces_count, token_span, heads_query, HEAD_SIZE),
        cosine_table,
        sine_table,
    ).astype(jnp.bfloat16)
    key = rotate(
        key_unrotated.reshape(pieces_count, token_span, heads_key, HEAD_SIZE),
        cosine_table,
        sine_table,
    ).astype(jnp.bfloat16)
    value = value_projected.reshape(pieces_count, token_span, heads_key, HEAD_SIZE).astype(
        jnp.bfloat16
    )
    d_attended = cotangent.reshape(pieces_count, token_span, heads_query, HEAD_SIZE)
    attended, query_back, key_rotated_back, value_returned = jax.vmap(segment_pass)(
        query, key, value, d_attended
    )
    attended_flat = attended.reshape(segment_length, heads_query * HEAD_SIZE)
    d_query = (
        inverse_rotation(query_back, cosine_table, sine_table)
        .astype(jnp.bfloat16)
        .reshape(segment_length, heads_query * HEAD_SIZE)
    )
    key_gradient = (
        inverse_rotation(key_rotated_back, cosine_table, sine_table)
        .astype(jnp.bfloat16)
        .reshape(segment_length, heads_key * HEAD_SIZE)
    )
    value_gradient = value_returned.astype(jnp.bfloat16).reshape(
        segment_length, heads_key * HEAD_SIZE
    )
    back_query, back_key, back_value = (
        lax.all_gather(w_query, "dp", axis=0, tiled=True),
        lax.all_gather(key_weight, "dp", axis=0, tiled=True),
        lax.all_gather(value_weight, "dp", axis=0, tiled=True),
    )
    joined = jnp.concatenate([d_query, key_gradient, value_gradient], 1)
    block = gathered
    grads = lax.psum_scatter(
        lax.dot_general(block, joined, contract_first, preferred_element_type=jnp.float32).astype(
            jnp.bfloat16
        ),
        "dp",
        scatter_dimension=0,
        tiled=True,
    ).astype(jnp.float32)
    width_query = w_query.shape[1]
    width_key = key_weight.shape[1]
    grad_query = grads[:, :width_query]
    grad_key = grads[:, width_query : width_query + width_key]
    grad_value = grads[:, width_query + width_key :]
    total = jnp.zeros((tokens.shape[0] * lax.axis_size("tensor"), gathered.shape[1]), jnp.float32)
    for grad_part, weight in (
        (d_query, back_query),
        (key_gradient, back_key),
        (value_gradient, back_value),
    ):
        block = grad_part
        total = total + lax.dot_general(
            block, weight, contract_last, preferred_element_type=jnp.float32
        )
    d_normed = lax.psum_scatter(
        total.astype(jnp.bfloat16), "tensor", scatter_dimension=0, tiled=True
    ).astype(jnp.float32)
    pre_part = jnp.sum(d_normed * unit_one, 0)
    scaled_in = d_normed * pre_gain
    grad_tokens = (
        inv_one * (scaled_in - unit_one * jnp.mean(scaled_in * unit_one, -1, keepdims=True))
    ).astype(jnp.bfloat16)
    grad_pre = lax.psum(pre_part, ("dp", "tensor"))
    return (attended_flat, grad_tokens, grad_query, grad_key, grad_value, grad_pre)


F32 = jnp.float32
BF16 = jnp.bfloat16
NN = (((1,), (0,)), ((), ()))
NT = (((1,), (1,)), ((), ()))
TN = (((0,), (0,)), ((), ()))


def swap_halves(values):
    half = values.shape[-1] // 2
    return jnp.concatenate([values[:, half:], values[:, :half]], -1)


def whole_kernel(
    dims,
    tok_hbm,
    gain_hbm,
    wq_ref,
    wk_ref,
    wv_ref,
    cot_hbm,
    cos_hbm,
    sin_hbm,
    mask_hbm,
    att_ref,
    gtok_ref,
    gq_ref,
    gk_ref,
    gv_ref,
    gpre_ref,
    tok_ref,
    gain_ref,
    cot_ref,
    cos_ref,
    sin_ref,
    mask_ref,
    x,
    xt,
    w,
    wt,
    proj,
    dproj,
    g,
    pr,
    dr,
    ar,
    dn,
    rb,
    pb1,
    pb2,
    ws,
    wr,
    xs,
    xr,
    ms,
    mr,
    gs,
    gr,
    zs,
    zr,
    ps,
    prs,
    ls,
    ins,
):
    n_dp, n_t, chunks, rep, hd, tile = dims
    dp = lax.axis_index("dp")
    t = lax.axis_index("tensor")
    rows = tok_ref.shape[0]
    width = tok_ref.shape[1]
    shard = wq_ref.shape[0]
    qw = rep * hd
    cw = qw + 2 * hd
    half = shard // 2
    n_chip = n_dp // 2
    parts = width // tile
    core = lax.rem(dp, 2)
    chip = lax.div(dp, 2)
    mate, px, py = dp ^ 1, dp ^ 2, dp ^ 4

    barrier = pltpu.get_barrier_semaphore()
    for o in range(1, n_dp):
        pl.semaphore_signal(
            barrier, inc=1, device_id=(dp ^ o, t), device_id_type=pl.DeviceIdType.MESH
        )
    for o in range(1, n_t):
        pl.semaphore_signal(
            barrier, inc=1, device_id=(dp, t ^ o), device_id_type=pl.DeviceIdType.MESH
        )

    loads = [
        pltpu.make_async_copy(src, dst, ins.at[i])
        for i, (src, dst) in enumerate(
            (
                (tok_hbm, tok_ref),
                (gain_hbm, gain_ref),
                (cos_hbm, cos_ref),
                (sin_hbm, sin_ref),
                (mask_hbm, mask_ref),
                (cot_hbm, cot_ref),
            )
        )
    ]

    def own_copies(j):
        here = pl.ds(pl.multiple_of(dp * shard, 16), shard)
        return (
            pltpu.make_async_copy(
                wq_ref.at[:, j * qw : (j + 1) * qw], w.at[j, here, 0:qw], ls.at[0, j]
            ),
            pltpu.make_async_copy(
                wk_ref.at[:, j * hd : (j + 1) * hd], w.at[j, here, qw : qw + hd], ls.at[1, j]
            ),
            pltpu.make_async_copy(
                wv_ref.at[:, j * hd : (j + 1) * hd], w.at[j, here, qw + hd : cw], ls.at[2, j]
            ),
        )

    loads[0].start()
    loads[1].start()
    for j in range(chunks):
        for copy in own_copies(j):
            copy.start()
    for copy in loads[2:]:
        copy.start()

    def rdma(src, dst, ssem, rsem, d, z):
        return pltpu.make_async_remote_copy(
            src_ref=src,
            dst_ref=dst,
            send_sem=ssem,
            recv_sem=rsem,
            device_id=(d, z),
            device_id_type=pl.DeviceIdType.MESH,
        )

    def wrow(who, h=None):
        if h is None:
            return pl.ds(pl.multiple_of(who * shard, 16), shard)
        return pl.ds(pl.multiple_of(who * shard + h * half, 16), half)

    def wcopy(kind, j, origin, to, h=None):
        place = w.at[j, wrow(origin, h)]
        return rdma(place, place, ws.at[kind, j], wr.at[kind, j], to, t)

    def offer(j):
        wcopy(0, j, dp, px).start()
        wcopy(1, j, dp, py).start()

    loads[0].wait()
    loads[1].wait()
    tokens = tok_ref[...].astype(F32)
    inv = lax.rsqrt(jnp.mean(tokens * tokens, -1, keepdims=True) + EPS)
    x[pl.ds(pl.multiple_of(t * rows, rows), rows), :] = (
        (tokens * inv) * gain_ref[...][None, :]
    ).astype(BF16)

    piece = rows // 2

    def xcopy(way, o, h, origin, to):
        place = x.at[pl.ds(pl.multiple_of(origin * rows + h * piece, piece), piece)]
        return rdma(place, place, xs.at[way, o, h], xr.at[way, o, h], dp, to)

    for copy in own_copies(0):
        copy.wait()
    pl.semaphore_wait(barrier, n_dp + n_t - 2)
    offer(0)

    @pl.when(t < n_t - 1)
    def _():
        for h in range(2):
            xcopy(0, 0, h, t, t + 1).start()

    @pl.when(t > 0)
    def _():
        for h in range(2):
            xcopy(1, 0, h, t, t - 1).start()

    for j in range(1, chunks):
        for copy in own_copies(j):
            copy.wait()
        if j < 2:
            offer(j)
    for j in range(chunks):
        wcopy(2, j, dp, mate).start()
    for copy in loads[2:]:
        copy.wait()

    def relay(j):
        wcopy(0, j, px, px).wait_recv()
        wcopy(5, j, px, py, h=0).start()
        wcopy(3, j, px, mate).start()
        wcopy(1, j, py, py).wait_recv()
        wcopy(6, j, py, px, h=1).start()
        wcopy(4, j, py, mate).start()

    def xrelay(o, h):
        @pl.when(t - o >= 0)
        def _():
            xcopy(0, o - 1, h, t - o, t).wait_recv()

            @pl.when(t + 1 < n_t)
            def _():
                xcopy(0, o, h, t - o, t + 1).start()

        @pl.when(t + o < n_t)
        def _():
            xcopy(1, o - 1, h, t + o, t).wait_recv()

            @pl.when(t > 0)
            def _():
                xcopy(1, o, h, t + o, t - 1).start()

    def far(j):
        wcopy(5, j, dp ^ 6, py, h=0).wait_recv()
        wcopy(6, j, dp ^ 6, px, h=1).wait_recv()
        wcopy(7, j, dp ^ 6, mate).start()

    def ready(j, relayed=False):
        if not relayed:
            far(j)
        wcopy(2, j, mate, mate).wait_recv()
        wcopy(3, j, dp ^ 3, mate).wait_recv()
        wcopy(4, j, dp ^ 5, mate).wait_recv()
        wcopy(7, j, dp ^ 7, mate).wait_recv()

    factor = query_scalar ** (-0.5)
    low = t < n_t // 2
    sign = jnp.where(low, 1, -1)
    m = jnp.where(low, t, n_t - 1 - t)
    fwd = jnp.where(low, 0, 1)

    def mirror(b):
        return jnp.where(low, b, n_t - 1 - b)

    places = (
        t,
        jnp.where(m == 0, t + sign, t - sign),
        jnp.where(m == 0, t + 2 * sign, t + sign),
        mirror(n_t - 1),
    )

    def head_cols(j, i):
        return pl.ds(pl.multiple_of(j * qw + i * hd, hd), hd)

    def block_rows(b, count=1):
        return pl.ds(pl.multiple_of(b * rows, rows), count * rows)

    def tiles(*which):
        for slot, (j, p) in enumerate(which):
            here = block_rows(places[p])
            proj[slot] = lax.dot_general(x[here, :], w[j], NN, preferred_element_type=F32)
        for slot, (j, p) in enumerate(which):
            here = block_rows(places[p])
            cosv, sinv = cos_ref[...], sin_ref[...]

            def turn(v):
                return v * cosv + swap_halves(v) * sinv

            def unturn(v):
                return v * cosv - swap_halves(v) * sinv

            q = jnp.concatenate(
                [turn(proj[slot, :, i * hd : (i + 1) * hd]).astype(BF16) for i in range(rep)], 0
            )
            k = turn(proj[slot, :, qw : qw + hd]).astype(BF16)
            v = proj[slot, :, qw + hd : cw].astype(BF16)
            cot = jnp.concatenate(
                [cot_ref[here, head_cols(j, i)] for i in range(rep)], 0
            )
            bent = jnp.tanh(
                lax.dot_general(q, k, NT, preferred_element_type=F32) * factor / CAP
            )
            raised = jnp.exp(CAP * bent) * mask_ref[...]
            weights = raised / jnp.sum(raised, -1, keepdims=True)
            probs = weights.astype(BF16)
            att = lax.dot_general(probs, v, NN, preferred_element_type=F32).astype(BF16)
            d_probs = lax.dot_general(cot, v, NT, preferred_element_type=F32)
            d_capped = weights * (d_probs - jnp.sum(weights * d_probs, -1, keepdims=True))
            ds = (d_capped * (1.0 - bent * bent) * factor).astype(BF16)
            dq = lax.dot_general(ds, k, NN, preferred_element_type=F32)
            dk = lax.dot_general(ds, q, TN, preferred_element_type=F32)
            dv = lax.dot_general(probs, cot, TN, preferred_element_type=F32)
            for i in range(rep):
                part = slice(i * rows, (i + 1) * rows)
                att_ref[here, head_cols(j, i)] = att[part]
                dproj[j, here, i * hd : (i + 1) * hd] = unturn(dq[part]).astype(BF16)
            dproj[j, here, qw : qw + hd] = unturn(dk).astype(BF16)
            dproj[j, here, qw + hd : cw] = dv.astype(BF16)

    def flip_rows(p):
        here = block_rows(places[p])
        xt[:, here] = x[here, :].T

    def flip_weights(j):
        wt[j] = w[j].T

    def span(p):
        return pl.ds(pl.multiple_of(p * tile, tile), tile)

    def zcopy(way, b, p, to):
        return rdma(
            dn.at[block_rows(b), span(p)],
            rb.at[way, b, :, span(p)],
            zs.at[way, b, p],
            zr.at[way, b, p],
            dp,
            to,
        )

    def outward(b, p):
        zcopy(fwd, mirror(b), p, t + sign).start()

    def back(first, count, sent):
        here = block_rows(first, count)

        def cols(p, c2):
            total = lax.dot_general(
                dproj[0, here, :], wt[0, :, span(p)], NN, preferred_element_type=F32
            )
            for j in range(1, chunks):
                total += lax.dot_general(
                    dproj[j, here, :], wt[j, :, span(p)], NN, preferred_element_type=F32
                )
            dn[here, span(p)] = total.astype(BF16)

            @pl.when(m == 0)
            def _():
                outward(sent, p)

            return c2

        lax.fori_loop(0, parts, cols, 0)

    strip = 64

    def gain_part(first, count, fresh):
        def cols(p, c2):
            def step(r, acc):
                here = pl.ds(pl.multiple_of(first * rows + r * strip, strip), strip)
                both = dn[here, span(p)].astype(F32) * x[here, span(p)].astype(F32)
                return acc + jnp.sum(both.reshape(strip // 8, 8, tile), 0)

            acc = lax.fori_loop(0, count * rows // strip, step, jnp.zeros((8, tile), F32))
            total = jnp.sum(acc, 0, keepdims=True)
            if not fresh:
                total = total + pb1[dp, :, span(p)]
            pb1[dp, :, span(p)] = total
            return c2

        lax.fori_loop(0, parts, cols, 0)

    lo, hi = pl.ds(0, half), pl.ds(half, half)

    def to_mate(j, i):
        return rdma(g.at[j, i, 0], pr.at[j, i], ms.at[j, i], mr.at[j, i], mate, t)

    def gcopy(kind, j, src, dst, to):
        return rdma(src, dst, gs.at[kind, j], gr.at[kind, j], to, t)

    def d_x(j):
        return gcopy(0, j, pr.at[j, 0, lo], dr.at[j, lo], px)

    def d_y(j):
        return gcopy(1, j, pr.at[j, 0, hi], dr.at[j, hi], py)

    def x_lo(j):
        return gcopy(2, j, pr.at[j, 2, lo], ar.at[0, j, lo], px)

    def x_hi(j):
        return gcopy(3, j, pr.at[j, 2, hi], ar.at[0, j, hi], px)

    def y_lo(j):
        return gcopy(4, j, pr.at[j, 1, lo], ar.at[1, j, lo], py)

    def y_hi(j):
        return gcopy(5, j, pr.at[j, 1, hi], ar.at[1, j, hi], py)

    def add(*terms):
        total = terms[0].astype(F32)
        for term in terms[1:]:
            total = total + term.astype(F32)
        return total.astype(BF16)

    def product(j, first=0, last=n_chip):
        def share(i, c2):
            c = chip ^ (n_chip - 1 - i)
            for k, who in enumerate((2 * c + 1 - core, 2 * c + core)):
                here = pl.ds(pl.multiple_of(who * shard, 16), shard)
                g[j, i, k] = lax.dot_general(
                    xt[here, :], dproj[j], NN, preferred_element_type=F32
                ).astype(BF16)
                if k == 0:
                    to_mate(j, i).start()
            return c2

        lax.fori_loop(first, last, share, 0)

    def joined(j, i):
        to_mate(j, i).wait_recv()
        pr[j, i] = add(g[j, i, 1], pr[j, i])

    def on_chip_far(j):
        joined(j, 0)
        d_x(j).start()
        d_y(j).start()

    def on_chip_near(j):
        joined(j, 1)
        y_hi(j).start()
        joined(j, 2)
        x_lo(j).start()

    def pass_on(j):
        d_x(j).wait_recv()
        pr[j, 1, lo] = add(pr[j, 1, lo], dr[j, lo])
        y_lo(j).start()
        d_y(j).wait_recv()
        pr[j, 2, hi] = add(pr[j, 2, hi], dr[j, hi])
        x_hi(j).start()

    def zsum(way, b, p):
        here = block_rows(b)
        cols = slice(p * tile, (p + 1) * tile)
        zcopy(way, b, p, t).wait_recv()
        dn[here, cols] = add(dn[here, cols], rb[way, b, :, cols])

    far_block = mirror(n_t - 1)
    rest = jnp.where(low, 0, 1)

    def pass_far(p):
        @pl.when(m > 0)
        def _():
            zsum(fwd, far_block, p)
            outward(n_t - 1, p)

    def pass_inner(p):
        @pl.when(m > 0)
        def _():
            zsum(1 - fwd, mirror(0), p)
            zcopy(1 - fwd, mirror(0), p, t - sign).start()

    def pass_next(p):
        @pl.when(m > 0)
        def _():
            zsum(fwd, mirror(n_t - 2), p)
            outward(n_t - 2, p)

    def p1(o):
        return rdma(pb1.at[dp], pb1.at[dp], ps.at[0, o], prs.at[0, o], dp ^ o, t)

    def p2(o):
        return rdma(pb2.at[t], pb2.at[t], ps.at[1, o], prs.at[1, o], dp, t ^ o)

    def p1r(o):
        return rdma(pb1.at[dp ^ o], pb1.at[dp ^ o], ps.at[0, o], prs.at[0, o], dp ^ o, t)

    def p2r(o):
        return rdma(pb2.at[t ^ o], pb2.at[t ^ o], ps.at[1, o], prs.at[1, o], dp, t ^ o)

    relay(0)
    offer(2)
    xrelay(1, 0)
    flip_rows(0)
    relay(1)
    offer(3)
    xrelay(1, 1)
    ready(0)
    tiles((0, 0), (0, 1))
    xrelay(2, 0)
    relay(2)
    flip_rows(1)
    flip_weights(0)
    ready(1)
    xrelay(2, 1)
    tiles((1, 0), (1, 1))
    tiles((0, 2), (1, 2))
    flip_rows(2)
    relay(3)
    flip_weights(1)
    ready(2)
    flip_weights(2)
    tiles((2, 0), (2, 1))
    xrelay(3, 0)
    xrelay(3, 1)
    tiles((0, 3))
    flip_rows(3)
    far(3)
    product(0, 0, 1)
    ready(3, True)
    tiles((1, 3), (2, 3), (3, 3))
    on_chip_far(0)
    flip_weights(3)
    back(far_block, 1, n_t - 1)
    product(0, 1)
    product(1)
    on_chip_near(0)
    pass_on(0)
    on_chip_far(1)
    on_chip_near(1)
    tiles((2, 2), (3, 2))
    tiles((3, 0), (3, 1))
    back(rest, n_t - 1, n_t - 2)

    @pl.when(m == 0)
    def _():
        for p in range(parts):
            outward(1, p)

    gain_part(rest, n_t - 1, True)
    gain_part(far_block, 1, False)
    pb1[dp] = pb1[dp] / gain_ref[...][None, :]
    for o in range(1, n_dp):
        p1(o).start()
    pass_far(0)
    product(2)
    pass_far(1)
    on_chip_far(2)
    on_chip_near(2)
    pass_far(2)
    pass_on(1)
    product(3)
    pass_inner(0)
    on_chip_far(3)
    on_chip_near(3)
    pass_inner(1)
    pass_next(0)
    pass_inner(2)
    for o in range(1, n_dp):
        p1r(o).wait_recv()
    total = pb1[0]
    for o in range(1, n_dp):
        total = total + pb1[o]
    pb2[t] = total
    for o in range(1, n_t):
        p2(o).start()
    pass_on(2)
    pass_next(1)
    for j in range(chunks):
        joined(j, 3)
    pass_next(2)
    pass_on(3)
    for o in range(1, n_t):
        p2r(o).wait_recv()
    total = pb2[0]
    for o in range(1, n_t):
        total = total + pb2[o]
    gpre_ref[...] = total[0]

    def final(j):
        x_lo(j).wait_recv()
        y_hi(j).wait_recv()
        y_lo(j).wait_recv()
        x_hi(j).wait_recv()
        done = add(pr[j, 3], ar[0, j], ar[1, j])
        gq_ref[:, j * qw : (j + 1) * qw] = done[:, :qw]
        gk_ref[:, j * hd : (j + 1) * hd] = done[:, qw : qw + hd]
        gv_ref[:, j * hd : (j + 1) * hd] = done[:, qw + hd :]

    for j in range(chunks - 1):
        final(j)

    mine = block_rows(t)
    for p in range(parts):
        zcopy(1 - fwd, t, p, t).wait_recv()

    @pl.when(m > 0)
    def _():
        for p in range(parts):
            zcopy(fwd, t, p, t).wait_recv()

    @pl.when(m == 0)
    def _():
        rb[fwd, t] = jnp.zeros((rows, width), BF16)

    d_normed = dn[mine, :].astype(F32) + rb[0, t].astype(F32) + rb[1, t].astype(F32)
    tokens2 = tok_ref[...].astype(F32)
    inv2 = lax.rsqrt(jnp.mean(tokens2 * tokens2, -1, keepdims=True) + EPS)
    unit = tokens2 * inv2
    e = d_normed * gain_ref[...][None, :]
    gtok_ref[...] = (inv2 * (e - unit * jnp.mean(e * unit, -1, keepdims=True))).astype(BF16)
    final(chunks - 1)

    for j in range(chunks):
        wcopy(0, j, dp, px).wait_send()
        wcopy(1, j, dp, py).wait_send()
        wcopy(2, j, dp, mate).wait_send()
        wcopy(3, j, px, mate).wait_send()
        wcopy(4, j, py, mate).wait_send()
        wcopy(5, j, px, py, h=0).wait_send()
        wcopy(6, j, py, px, h=1).wait_send()
        wcopy(7, j, dp ^ 6, mate).wait_send()
        for i in range(n_chip):
            to_mate(j, i).wait_send()
        for copy in (d_x, d_y, x_lo, x_hi, y_lo, y_hi):
            copy(j).wait_send()
    for h in range(2):
        for o in range(n_t - 1):
            @pl.when((t - o >= 0) & (t + 1 < n_t))
            def _():
                xcopy(0, o, h, t - o, t + 1).wait_send()

            @pl.when((t + o < n_t) & (t > 0))
            def _():
                xcopy(1, o, h, t + o, t - 1).wait_send()

    for p in range(parts):
        for b in range(n_t - 1, 0, -1):
            @pl.when(m < b)
            def _():
                zcopy(fwd, mirror(b), p, t + sign).wait_send()

        @pl.when(m > 0)
        def _():
            zcopy(1 - fwd, mirror(0), p, t - sign).wait_send()

    for o in range(1, n_dp):
        p1(o).wait_send()
    for o in range(1, n_t):
        p2(o).wait_send()


def finish_kernel(att, gtok, gq, gk, gv, gpre, *refs):
    outs, (bq, bk, bv), sems = refs[:6], refs[6:9], refs[9]
    copies = [
        pltpu.make_async_copy(src, outs[i], sems.at[i])
        for src, i in ((att, 0), (gtok, 1), (bq, 2), (bk, 3), (bv, 4), (gpre, 5))
    ]
    for i in (0, 1, 5):
        copies[i].start()
    for src, wide, i in ((gq, bq, 2), (gk, bk, 3), (gv, bv, 4)):
        wide[...] = src[...].astype(F32)
        copies[i].start()
    for copy in copies:
        copy.wait()


def fused_per_device(tokens, cotangent, pre_gain, w_query, key_weight, value_weight):
    n_dp, n_t = lax.axis_size("dp"), lax.axis_size("tensor")
    rows, width = tokens.shape
    block = rows * n_t
    shard = w_query.shape[0]
    chunks = key_weight.shape[1] // HEAD_SIZE
    rep = w_query.shape[1] // key_weight.shape[1]
    qw = rep * HEAD_SIZE
    cw = qw + 2 * HEAD_SIZE
    kw = chunks * HEAD_SIZE
    half = HEAD_SIZE // 2
    parts = 3 if width % (3 * HEAD_SIZE) == 0 else 1
    n_chip = n_dp // 2
    place = np.arange(rows)
    freqs = BASE ** (-np.arange(half) / half)
    angles = (place % SEQ_LEN)[:, None] * freqs[None, :]
    cosine = np.concatenate([np.cos(angles)] * 2, -1).astype(np.float32)
    sine = np.concatenate([-np.sin(angles), np.sin(angles)], -1).astype(np.float32)
    mask = (place[None, :] <= place[:, None]) & (
        place[None, :] // SEQ_LEN == place[:, None] // SEQ_LEN
    )
    mask = np.tile(mask.astype(np.float32), (rep, 1))
    vmem = pl.BlockSpec(memory_space=pltpu.VMEM)
    hbm = pl.BlockSpec(memory_space=pl.ANY)
    dma = pltpu.SemaphoreType.DMA
    made = pl.pallas_call(
        functools.partial(whole_kernel, (n_dp, n_t, chunks, rep, HEAD_SIZE, width // parts)),
        out_shape=(
            pltpu.VMEM((block, chunks * qw), BF16),
            pltpu.VMEM((rows, width), BF16),
            pltpu.VMEM((shard, chunks * qw), BF16),
            pltpu.VMEM((shard, kw), BF16),
            pltpu.VMEM((shard, kw), BF16),
            pltpu.VMEM((width,), F32),
        ),
        in_specs=[hbm] * 9,
        out_specs=(vmem,) * 6,
        scratch_shapes=[
            pltpu.VMEM((rows, width), BF16),
            pltpu.VMEM((width,), F32),
            pltpu.VMEM((block, chunks * qw), BF16),
            pltpu.VMEM(cosine.shape, F32),
            pltpu.VMEM(sine.shape, F32),
            pltpu.VMEM(mask.shape, F32),
            pltpu.VMEM((block, width), BF16),
            pltpu.VMEM((width, block), BF16),
            pltpu.VMEM((chunks, width, cw), BF16),
            pltpu.VMEM((chunks, cw, width), BF16),
            pltpu.VMEM((3, rows, cw), F32),
            pltpu.VMEM((chunks, block, cw), BF16),
            pltpu.VMEM((chunks, n_chip, 2, shard, cw), BF16),
            pltpu.VMEM((chunks, n_chip, shard, cw), BF16),
            pltpu.VMEM((chunks, shard, cw), BF16),
            pltpu.VMEM((2, chunks, shard, cw), BF16),
            pltpu.VMEM((block, width), BF16),
            pltpu.VMEM((2, n_t, rows, width), BF16),
            pltpu.VMEM((n_dp, 1, width), F32),
            pltpu.VMEM((n_t, 1, width), F32),
            dma((8, chunks)),
            dma((8, chunks)),
            dma((2, n_t, 2)),
            dma((2, n_t, 2)),
            dma((chunks, n_chip)),
            dma((chunks, n_chip)),
            dma((6, chunks)),
            dma((6, chunks)),
            dma((2, n_t, parts)),
            dma((2, n_t, parts)),
            dma((2, n_dp)),
            dma((2, n_dp)),
            dma((3, chunks)),
            dma((6,)),
        ],
        compiler_params=pltpu.CompilerParams(
            collective_id=0, has_side_effects=True, vmem_limit_bytes=58 * 1024 * 1024
        ),
    )(tokens, pre_gain, w_query, key_weight, value_weight, cotangent, cosine, sine, mask)
    return pl.pallas_call(
        finish_kernel,
        out_shape=(
            jax.ShapeDtypeStruct((block, chunks * qw), BF16),
            jax.ShapeDtypeStruct((rows, width), BF16),
            jax.ShapeDtypeStruct((shard, chunks * qw), F32),
            jax.ShapeDtypeStruct((shard, kw), F32),
            jax.ShapeDtypeStruct((shard, kw), F32),
            jax.ShapeDtypeStruct((width,), F32),
        ),
        in_specs=[vmem] * 6,
        out_specs=(hbm,) * 6,
        scratch_shapes=[
            pltpu.VMEM((shard, chunks * qw), F32),
            pltpu.VMEM((shard, kw), F32),
            pltpu.VMEM((shard, kw), F32),
            dma((6,)),
        ],
        compiler_params=pltpu.CompilerParams(vmem_limit_bytes=16 * 1024 * 1024),
    )(*made)


def solution(mesh):
    fused = mesh.shape["dp"] == 8 and mesh.shape["tensor"] == 4
    placed = (
        P(("dp", "tensor"), None),
        P("dp", "tensor"),
        P(),
        P("dp", "tensor"),
        P("dp", "tensor"),
        P("dp", "tensor"),
    )
    return jax.shard_map(
        fused_per_device if fused else per_device,
        mesh=mesh,
        in_specs=placed,
        out_specs=(
            P("dp", "tensor"),
            P(("dp", "tensor"), None),
            P("dp", "tensor"),
            P("dp", "tensor"),
            P("dp", "tensor"),
            P(),
        ),
        check_vma=False,
    )
```

```python
import functools

import jax
import jax.numpy as jnp
import numpy as np
from jax import lax
from jax.experimental import pallas as pl
from jax.experimental.pallas import tpu as pltpu
from jax.sharding import PartitionSpec as P

HEAD_SIZE = 128
SEQ_LEN = 64


EPS = 1e-06
CAP = 50.0
BASE = 10000.0
query_scalar = 144.0


def rotary_tables(segment_length, half):
    places = jnp.arange(segment_length, dtype=jnp.float32)[:, None]
    freqs = BASE ** (-jnp.arange(half, dtype=jnp.float32) / half)
    angles = places * freqs[None, :]
    return (jnp.cos(angles)[:, None, :], jnp.sin(angles)[:, None, :])


def rotate(values, cosine_table, sine_table):
    half = values.shape[-1] // 2
    first, second = (values[..., :half], values[..., half:])
    return jnp.concatenate(
        [first * cosine_table - second * sine_table, second * cosine_table + first * sine_table], -1
    )


def inverse_rotation(values, cosine_table, sine_table):
    half = values.shape[-1] // 2
    first, second = (values[..., :half], values[..., half:])
    return jnp.concatenate(
        [first * cosine_table + second * sine_table, second * cosine_table - first * sine_table], -1
    )


def attend_forward(query, key, value):
    repeat = query.shape[1] // key.shape[1]
    keys = jnp.repeat(key, repeat, axis=1)
    values = jnp.repeat(value, repeat, axis=1)
    factor = query_scalar ** (-0.5)
    raw = jnp.einsum("qhd,khd->hqk", query, keys, preferred_element_type=jnp.float32) * factor
    bent = jnp.tanh(raw / CAP)
    capped = CAP * bent
    segment_length = query.shape[0]
    causal = jnp.arange(segment_length)[None, :] <= jnp.arange(segment_length)[:, None]
    raised = jnp.where(causal[None], jnp.exp(capped), 0.0)
    weights = raised / jnp.sum(raised, -1, keepdims=True)
    probs = weights.astype(jnp.bfloat16)
    attended = jnp.einsum("hqk,khd->qhd", probs, values, preferred_element_type=jnp.float32).astype(
        jnp.bfloat16
    )
    return (attended, weights, probs, bent)


def attend_backward(d_attended, query, key, value, weights, probs, bent):
    repeat = query.shape[1] // key.shape[1]
    keys = jnp.repeat(key, repeat, axis=1)
    values = jnp.repeat(value, repeat, axis=1)
    factor = query_scalar ** (-0.5)
    d_probs = jnp.einsum("qhd,khd->hqk", d_attended, values, preferred_element_type=jnp.float32)
    d_capped = weights * (d_probs - jnp.sum(weights * d_probs, -1, keepdims=True))
    d_scores = (d_capped * (1.0 - bent * bent) * factor).astype(jnp.bfloat16)
    query_back = jnp.einsum("hqk,khd->qhd", d_scores, keys, preferred_element_type=jnp.float32)
    key_heads = jnp.einsum("hqk,qhd->khd", d_scores, query, preferred_element_type=jnp.float32)
    value_heads = jnp.einsum("hqk,qhd->khd", probs, d_attended, preferred_element_type=jnp.float32)
    segment_length, heads, width = query.shape
    key_rotated_back = key_heads.reshape(segment_length, heads // repeat, repeat, width).sum(2)
    value_returned = value_heads.reshape(segment_length, heads // repeat, repeat, width).sum(2)
    return (query_back, key_rotated_back, value_returned)


def segment_pass(query, key, value, d_attended):
    attended, weights, probs, bent = attend_forward(query, key, value)
    query_back, key_rotated_back, value_returned = attend_backward(
        d_attended, query, key, value, weights, probs, bent
    )
    return (attended, query_back, key_rotated_back, value_returned)


def per_device(tokens, cotangent, pre_gain, w_query, key_weight, value_weight):
    contract_first = (((0,), (0,)), ((), ()))
    contract_last = (((1,), (1,)), ((), ()))
    rows_f = tokens.astype(jnp.float32)
    inv_one = lax.rsqrt(jnp.mean(rows_f * rows_f, -1, keepdims=True) + EPS)
    unit_one = rows_f * inv_one
    normed_input = (unit_one * pre_gain).astype(jnp.bfloat16)
    gathered = lax.all_gather(normed_input, "tensor", axis=0, tiled=True)
    segment_length = gathered.shape[0]
    token_span = SEQ_LEN
    pieces_count = segment_length // token_span
    heads_query = w_query.shape[1] // HEAD_SIZE
    heads_key = key_weight.shape[1] // HEAD_SIZE
    pieces = (
        lax.all_gather(w_query, "dp", axis=0, tiled=True),
        lax.all_gather(key_weight, "dp", axis=0, tiled=True),
        lax.all_gather(value_weight, "dp", axis=0, tiled=True),
    )
    query_raw, key_unrotated, value_projected = tuple(
        (jnp.dot(gathered, piece, preferred_element_type=jnp.float32) for piece in pieces)
    )
    cosine_table, sine_table = rotary_tables(token_span, HEAD_SIZE // 2)
    query = rotate(
        query_raw.reshape(pieces_count, token_span, heads_query, HEAD_SIZE),
        cosine_table,
        sine_table,
    ).astype(jnp.bfloat16)
    key = rotate(
        key_unrotated.reshape(pieces_count, token_span, heads_key, HEAD_SIZE),
        cosine_table,
        sine_table,
    ).astype(jnp.bfloat16)
    value = value_projected.reshape(pieces_count, token_span, heads_key, HEAD_SIZE).astype(
        jnp.bfloat16
    )
    d_attended = cotangent.reshape(pieces_count, token_span, heads_query, HEAD_SIZE)
    attended, query_back, key_rotated_back, value_returned = jax.vmap(segment_pass)(
        query, key, value, d_attended
    )
    attended_flat = attended.reshape(segment_length, heads_query * HEAD_SIZE)
    d_query = (
        inverse_rotation(query_back, cosine_table, sine_table)
        .astype(jnp.bfloat16)
        .reshape(segment_length, heads_query * HEAD_SIZE)
    )
    key_gradient = (
        inverse_rotation(key_rotated_back, cosine_table, sine_table)
        .astype(jnp.bfloat16)
        .reshape(segment_length, heads_key * HEAD_SIZE)
    )
    value_gradient = value_returned.astype(jnp.bfloat16).reshape(
        segment_length, heads_key * HEAD_SIZE
    )
    back_query, back_key, back_value = (
        lax.all_gather(w_query, "dp", axis=0, tiled=True),
        lax.all_gather(key_weight, "dp", axis=0, tiled=True),
        lax.all_gather(value_weight, "dp", axis=0, tiled=True),
    )
    joined = jnp.concatenate([d_query, key_gradient, value_gradient], 1)
    block = gathered
    grads = lax.psum_scatter(
        lax.dot_general(block, joined, contract_first, preferred_element_type=jnp.float32).astype(
            jnp.bfloat16
        ),
        "dp",
        scatter_dimension=0,
        tiled=True,
    ).astype(jnp.float32)
    width_query = w_query.shape[1]
    width_key = key_weight.shape[1]
    grad_query = grads[:, :width_query]
    grad_key = grads[:, width_query : width_query + width_key]
    grad_value = grads[:, width_query + width_key :]
    total = jnp.zeros((tokens.shape[0] * lax.axis_size("tensor"), gathered.shape[1]), jnp.float32)
    for grad_part, weight in (
        (d_query, back_query),
        (key_gradient, back_key),
        (value_gradient, back_value),
    ):
        block = grad_part
        total = total + lax.dot_general(
            block, weight, contract_last, preferred_element_type=jnp.float32
        )
    d_normed = lax.psum_scatter(
        total.astype(jnp.bfloat16), "tensor", scatter_dimension=0, tiled=True
    ).astype(jnp.float32)
    pre_part = jnp.sum(d_normed * unit_one, 0)
    scaled_in = d_normed * pre_gain
    grad_tokens = (
        inv_one * (scaled_in - unit_one * jnp.mean(scaled_in * unit_one, -1, keepdims=True))
    ).astype(jnp.bfloat16)
    grad_pre = lax.psum(pre_part, ("dp", "tensor"))
    return (attended_flat, grad_tokens, grad_query, grad_key, grad_value, grad_pre)


F32 = jnp.float32
BF16 = jnp.bfloat16
NN = (((1,), (0,)), ((), ()))
NT = (((1,), (1,)), ((), ()))
TN = (((0,), (0,)), ((), ()))


def swap_halves(values):
    half = values.shape[-1] // 2
    return jnp.concatenate([values[:, half:], values[:, :half]], -1)


def whole_kernel(
    dims,
    tok_hbm,
    gain_hbm,
    wq_ref,
    wk_ref,
    wv_ref,
    cot_hbm,
    cos_hbm,
    sin_hbm,
    mask_hbm,
    att_ref,
    gtok_ref,
    gq_ref,
    gk_ref,
    gv_ref,
    gpre_ref,
    tok_ref,
    gain_ref,
    cot_ref,
    cos_ref,
    sin_ref,
    mask_ref,
    x,
    xt,
    w,
    wt,
    proj,
    dproj,
    g,
    pr,
    dr,
    ar,
    dn,
    rb,
    pb1,
    pb2,
    ws,
    wr,
    xs,
    xr,
    qs,
    qr,
    ms,
    mr,
    gs,
    gr,
    zs,
    zr,
    ps,
    prs,
    ls,
    ins,
):
    n_dp, n_t, chunks, rep, hd, tile = dims
    dp = lax.axis_index("dp")
    t = lax.axis_index("tensor")
    rows = tok_ref.shape[0]
    width = tok_ref.shape[1]
    shard = wq_ref.shape[0]
    qw = rep * hd
    cw = qw + 2 * hd
    half = shard // 2
    n_chip = n_dp // 2
    parts = width // tile
    core = lax.rem(dp, 2)
    chip = lax.div(dp, 2)
    mate, px, py = dp ^ 1, dp ^ 2, dp ^ 4

    barrier = pltpu.get_barrier_semaphore()

    def greet(d, z):
        pl.semaphore_signal(
            barrier, inc=1, device_id=(d, z), device_id_type=pl.DeviceIdType.MESH
        )

    greet(px, t)
    greet(py, t)

    @pl.when(t < n_t - 1)
    def _():
        greet(dp, t + 1)

    @pl.when(t > 0)
    def _():
        greet(dp, t - 1)

    greet(mate, t)

    loads = [
        pltpu.make_async_copy(src, dst, ins.at[i])
        for i, (src, dst) in enumerate(
            (
                (tok_hbm, tok_ref),
                (gain_hbm, gain_ref),
                (cos_hbm, cos_ref),
                (sin_hbm, sin_ref),
                (mask_hbm, mask_ref),
                (cot_hbm, cot_ref),
            )
        )
    ]

    def own_copies(j):
        here = pl.ds(pl.multiple_of(dp * shard, 16), shard)
        return (
            pltpu.make_async_copy(
                wq_ref.at[:, j * qw : (j + 1) * qw], w.at[j, here, 0:qw], ls.at[0, j]
            ),
            pltpu.make_async_copy(
                wk_ref.at[:, j * hd : (j + 1) * hd], w.at[j, here, qw : qw + hd], ls.at[1, j]
            ),
            pltpu.make_async_copy(
                wv_ref.at[:, j * hd : (j + 1) * hd], w.at[j, here, qw + hd : cw], ls.at[2, j]
            ),
        )

    loads[0].start()
    loads[1].start()
    for j in range(chunks):
        for copy in own_copies(j):
            copy.start()
    for copy in loads[2:]:
        copy.start()

    def rdma(src, dst, ssem, rsem, d, z):
        return pltpu.make_async_remote_copy(
            src_ref=src,
            dst_ref=dst,
            send_sem=ssem,
            recv_sem=rsem,
            device_id=(d, z),
            device_id_type=pl.DeviceIdType.MESH,
        )

    def wrow(who, h=None):
        if h is None:
            return pl.ds(pl.multiple_of(who * shard, 16), shard)
        return pl.ds(pl.multiple_of(who * shard + h * half, 16), half)

    def wcopy(kind, j, origin, to, h=None):
        place = w.at[j, wrow(origin, h)]
        return rdma(place, place, ws.at[kind, j], wr.at[kind, j], to, t)

    def offer(j):
        wcopy(0, j, dp, px).start()
        wcopy(1, j, dp, py).start()

    low = t < n_t // 2
    sign = jnp.where(low, 1, -1)
    m = jnp.where(low, t, n_t - 1 - t)
    fwd = jnp.where(low, 0, 1)
    piece, quarter = rows // 2, rows // 4

    def xcopy(way, o, h, origin, to):
        place = x.at[pl.ds(pl.multiple_of(origin * rows + h * piece, piece), piece)]
        return rdma(place, place, xs.at[way, o, h], xr.at[way, o, h], dp, to)

    def qcopy(k, origin, to):
        first = pl.multiple_of(origin * rows + piece + k * quarter, quarter)
        place = x.at[pl.ds(first, quarter)]
        return rdma(place, place, qs.at[k], qr.at[k], dp, to)

    for copy in own_copies(0):
        copy.wait()
    pl.semaphore_wait(barrier, 3 + jnp.where(m == 0, 1, 2))
    offer(0)
    for copy in own_copies(1):
        copy.wait()
    offer(1)
    loads[0].wait()
    loads[1].wait()
    tokens = tok_ref[...].astype(F32)
    inv = lax.rsqrt(jnp.mean(tokens * tokens, -1, keepdims=True) + EPS)
    x[pl.ds(pl.multiple_of(t * rows, rows), rows), :] = (
        (tokens * inv) * gain_ref[...][None, :]
    ).astype(BF16)

    @pl.when(t < n_t - 1)
    def _():
        xcopy(0, 0, 0, t, t + 1).start()

    @pl.when(t > 0)
    def _():
        xcopy(1, 0, 0, t, t - 1).start()

    @pl.when(t < n_t - 2)
    def _():
        xcopy(0, 0, 1, t, t + 1).start()

    @pl.when(t > 1)
    def _():
        xcopy(1, 0, 1, t, t - 1).start()

    @pl.when(m > 0)
    def _():
        qcopy(0, t, t - sign).start()

    for j in range(2, chunks):
        for copy in own_copies(j):
            copy.wait()
    for j in range(chunks):
        wcopy(2, j, dp, mate).start()
    for copy in loads[2:]:
        copy.wait()

    def relay(j):
        wcopy(0, j, px, px).wait_recv()
        wcopy(5, j, px, py, h=0).start()
        wcopy(3, j, px, mate).start()
        wcopy(1, j, py, py).wait_recv()
        wcopy(6, j, py, px, h=1).start()
        wcopy(4, j, py, mate).start()

    def xrelay(o, h):
        split = o == 1 and h == 1
        above = (t - o >= 0) & (t < n_t - 1) if split else t - o >= 0
        below = (t + o < n_t) & (t > 0) if split else t + o < n_t

        @pl.when(above)
        def _():
            xcopy(0, o - 1, h, t - o, t).wait_recv()

            @pl.when(t + 1 < n_t)
            def _():
                xcopy(0, o, h, t - o, t + 1).start()

        @pl.when(below)
        def _():
            xcopy(1, o - 1, h, t + o, t).wait_recv()

            @pl.when(t > 0)
            def _():
                xcopy(1, o, h, t + o, t - 1).start()

    def xlate():
        @pl.when(m > 0)
        def _():
            qcopy(1, t, t - sign).start()

    def xfinish():
        @pl.when(m == 0)
        def _():
            for k in range(2):
                qcopy(k, t + sign, t).wait_recv()

    def far(j):
        wcopy(5, j, dp ^ 6, py, h=0).wait_recv()
        wcopy(6, j, dp ^ 6, px, h=1).wait_recv()
        wcopy(7, j, dp ^ 6, mate).start()

    def ready(j, relayed=False):
        if not relayed:
            far(j)
        wcopy(2, j, mate, mate).wait_recv()
        wcopy(3, j, dp ^ 3, mate).wait_recv()
        wcopy(4, j, dp ^ 5, mate).wait_recv()
        wcopy(7, j, dp ^ 7, mate).wait_recv()

    factor = query_scalar ** (-0.5)

    def mirror(b):
        return jnp.where(low, b, n_t - 1 - b)

    places = (
        t,
        jnp.where(m == 0, t + sign, t - sign),
        jnp.where(m == 0, t + 2 * sign, t + sign),
        mirror(n_t - 1),
    )

    def head_cols(j, i):
        return pl.ds(pl.multiple_of(j * qw + i * hd, hd), hd)

    def block_rows(b, count=1):
        return pl.ds(pl.multiple_of(b * rows, rows), count * rows)

    def tiles(*which):
        for slot, (j, p) in enumerate(which):
            here = block_rows(places[p])
            proj[slot] = lax.dot_general(x[here, :], w[j], NN, preferred_element_type=F32)
        for slot, (j, p) in enumerate(which):
            here = block_rows(places[p])
            cosv, sinv = cos_ref[...], sin_ref[...]

            def turn(v):
                return v * cosv + swap_halves(v) * sinv

            def unturn(v):
                return v * cosv - swap_halves(v) * sinv

            q = jnp.concatenate(
                [turn(proj[slot, :, i * hd : (i + 1) * hd]).astype(BF16) for i in range(rep)], 0
            )
            k = turn(proj[slot, :, qw : qw + hd]).astype(BF16)
            v = proj[slot, :, qw + hd : cw].astype(BF16)
            cot = jnp.concatenate(
                [cot_ref[here, head_cols(j, i)] for i in range(rep)], 0
            )
            bent = jnp.tanh(
                lax.dot_general(q, k, NT, preferred_element_type=F32) * factor / CAP
            )
            raised = jnp.exp(CAP * bent) * mask_ref[...]
            weights = raised / jnp.sum(raised, -1, keepdims=True)
            probs = weights.astype(BF16)
            att = lax.dot_general(probs, v, NN, preferred_element_type=F32).astype(BF16)
            d_probs = lax.dot_general(cot, v, NT, preferred_element_type=F32)
            d_capped = weights * (d_probs - jnp.sum(weights * d_probs, -1, keepdims=True))
            ds = (d_capped * (1.0 - bent * bent) * factor).astype(BF16)
            dq = lax.dot_general(ds, k, NN, preferred_element_type=F32)
            dk = lax.dot_general(ds, q, TN, preferred_element_type=F32)
            dv = lax.dot_general(probs, cot, TN, preferred_element_type=F32)
            for i in range(rep):
                part = slice(i * rows, (i + 1) * rows)
                att_ref[here, head_cols(j, i)] = att[part]
                dproj[j, here, i * hd : (i + 1) * hd] = unturn(dq[part]).astype(BF16)
            dproj[j, here, qw : qw + hd] = unturn(dk).astype(BF16)
            dproj[j, here, qw + hd : cw] = dv.astype(BF16)

    def flip_rows(p):
        here = block_rows(places[p])
        xt[:, here] = x[here, :].T

    def flip_weights(j):
        wt[j] = w[j].T

    def span(p):
        return pl.ds(pl.multiple_of(p * tile, tile), tile)

    def zcopy(way, b, p, to):
        return rdma(
            dn.at[block_rows(b), span(p)],
            rb.at[way, b, :, span(p)],
            zs.at[way, b, p],
            zr.at[way, b, p],
            dp,
            to,
        )

    def outward(b, p):
        zcopy(fwd, mirror(b), p, t + sign).start()

    def back(first, count, sent):
        here = block_rows(first, count)

        def cols(p, c2):
            total = lax.dot_general(
                dproj[0, here, :], wt[0, :, span(p)], NN, preferred_element_type=F32
            )
            for j in range(1, chunks):
                total += lax.dot_general(
                    dproj[j, here, :], wt[j, :, span(p)], NN, preferred_element_type=F32
                )
            dn[here, span(p)] = total.astype(BF16)

            @pl.when(m == 0)
            def _():
                outward(sent, p)

            return c2

        lax.fori_loop(0, parts, cols, 0)

    strip = 64

    def gain_part(first, count, fresh):
        def cols(p, c2):
            def step(r, acc):
                here = pl.ds(pl.multiple_of(first * rows + r * strip, strip), strip)
                both = dn[here, span(p)].astype(F32) * x[here, span(p)].astype(F32)
                return acc + jnp.sum(both.reshape(strip // 8, 8, tile), 0)

            acc = lax.fori_loop(0, count * rows // strip, step, jnp.zeros((8, tile), F32))
            total = jnp.sum(acc, 0, keepdims=True)
            if not fresh:
                total = total + pb1[t, :, span(p)]
            pb1[t, :, span(p)] = total
            return c2

        lax.fori_loop(0, parts, cols, 0)

    lo, hi = pl.ds(0, half), pl.ds(half, half)

    def to_mate(j, i):
        return rdma(g.at[j, i, 0], pr.at[j, i], ms.at[j, i], mr.at[j, i], mate, t)

    def gcopy(kind, j, src, dst, to):
        return rdma(src, dst, gs.at[kind, j], gr.at[kind, j], to, t)

    def d_x(j):
        return gcopy(0, j, pr.at[j, 0, lo], dr.at[j, lo], px)

    def d_y(j):
        return gcopy(1, j, pr.at[j, 0, hi], dr.at[j, hi], py)

    def x_lo(j):
        return gcopy(2, j, pr.at[j, 2, lo], ar.at[0, j, lo], px)

    def x_hi(j):
        return gcopy(3, j, pr.at[j, 2, hi], ar.at[0, j, hi], px)

    def y_lo(j):
        return gcopy(4, j, pr.at[j, 1, lo], ar.at[1, j, lo], py)

    def y_hi(j):
        return gcopy(5, j, pr.at[j, 1, hi], ar.at[1, j, hi], py)

    def add(*terms):
        total = terms[0].astype(F32)
        for term in terms[1:]:
            total = total + term.astype(F32)
        return total.astype(BF16)

    def product(j, first=0, last=n_chip):
        def share(i, c2):
            c = chip ^ (n_chip - 1 - i)
            for k, who in enumerate((2 * c + 1 - core, 2 * c + core)):
                here = pl.ds(pl.multiple_of(who * shard, 16), shard)
                g[j, i, k] = lax.dot_general(
                    xt[here, :], dproj[j], NN, preferred_element_type=F32
                ).astype(BF16)
                if k == 0:
                    to_mate(j, i).start()
            return c2

        lax.fori_loop(first, last, share, 0)

    def joined(j, i):
        to_mate(j, i).wait_recv()
        pr[j, i] = add(g[j, i, 1], pr[j, i])

    def on_chip_far(j):
        joined(j, 0)
        d_x(j).start()
        d_y(j).start()

    def on_chip_near(j):
        joined(j, 1)
        y_hi(j).start()
        joined(j, 2)
        x_lo(j).start()

    def pass_on(j):
        d_x(j).wait_recv()
        pr[j, 1, lo] = add(pr[j, 1, lo], dr[j, lo])
        y_lo(j).start()
        d_y(j).wait_recv()
        pr[j, 2, hi] = add(pr[j, 2, hi], dr[j, hi])
        x_hi(j).start()

    def zsum(way, b, p):
        here = block_rows(b)
        cols = slice(p * tile, (p + 1) * tile)
        zcopy(way, b, p, t).wait_recv()
        dn[here, cols] = add(dn[here, cols], rb[way, b, :, cols])

    far_block = mirror(n_t - 1)
    rest = jnp.where(low, 0, 1)

    def pass_far(p):
        @pl.when(m > 0)
        def _():
            zsum(fwd, far_block, p)
            outward(n_t - 1, p)

    def pass_inner(p):
        @pl.when(m > 0)
        def _():
            zsum(1 - fwd, mirror(0), p)
            zcopy(1 - fwd, mirror(0), p, t - sign).start()

    def pass_next(p):
        @pl.when(m > 0)
        def _():
            zsum(fwd, mirror(n_t - 2), p)
            outward(n_t - 2, p)

    def p1(o):
        return rdma(pb1.at[t], pb1.at[t], ps.at[0, o], prs.at[0, o], dp, t ^ o)

    def p2(o):
        return rdma(pb2.at[dp], pb2.at[dp], ps.at[1, o], prs.at[1, o], dp ^ o, t)

    def p1r(o):
        return rdma(pb1.at[t ^ o], pb1.at[t ^ o], ps.at[0, o], prs.at[0, o], dp, t ^ o)

    def p2r(o):
        return rdma(pb2.at[dp ^ o], pb2.at[dp ^ o], ps.at[1, o], prs.at[1, o], dp ^ o, t)

    def final(j):
        x_lo(j).wait_recv()
        y_hi(j).wait_recv()
        y_lo(j).wait_recv()
        x_hi(j).wait_recv()
        done = pr[j, 3].astype(F32) + ar[0, j].astype(F32) + ar[1, j].astype(F32)
        gq_ref[:, j * qw : (j + 1) * qw] = done[:, :qw]
        gk_ref[:, j * hd : (j + 1) * hd] = done[:, qw : qw + hd]
        gv_ref[:, j * hd : (j + 1) * hd] = done[:, qw + hd :]

    relay(0)
    offer(2)
    xrelay(1, 0)
    flip_rows(0)
    relay(1)
    offer(3)
    xrelay(1, 1)
    ready(0)
    tiles((0, 0))
    xrelay(2, 0)
    relay(2)
    flip_weights(0)
    ready(1)
    xrelay(2, 1)
    xlate()
    tiles((1, 0), (0, 2), (1, 2))
    flip_rows(2)
    relay(3)
    flip_weights(1)
    far(2)
    xrelay(3, 0)
    xrelay(3, 1)
    tiles((0, 3), (1, 3))
    flip_rows(3)
    ready(2, True)
    flip_weights(2)
    far(3)
    tiles((2, 3))
    xfinish()
    tiles((0, 1))
    flip_rows(1)
    product(0, 0, 1)
    ready(3, True)
    tiles((3, 3))
    on_chip_far(0)
    flip_weights(3)
    back(far_block, 1, n_t - 1)
    gain_part(far_block, 1, True)
    product(0, 1, 3)
    on_chip_near(0)
    tiles((1, 1))
    product(1, 0, 3)
    pass_on(0)
    on_chip_far(1)
    tiles((2, 0), (2, 1), (2, 2))
    on_chip_near(1)
    pass_far(0)
    tiles((3, 0), (3, 1), (3, 2))
    product(2, 0, 1)
    back(rest, n_t - 1, n_t - 2)
    on_chip_far(2)
    gain_part(rest, n_t - 1, False)
    pb1[t] = pb1[t] / gain_ref[...][None, :]
    for o in range(1, n_t):
        p1(o).start()

    @pl.when(m == 0)
    def _():
        for p in range(parts):
            outward(1, p)

    pass_on(1)
    pass_far(1)
    pass_far(2)
    product(2, 1, 3)
    on_chip_near(2)
    product(3, 0, 3)
    pass_inner(0)
    on_chip_far(3)
    product(0, 3, 4)
    product(1, 3, 4)
    on_chip_near(3)
    pass_inner(1)
    pass_next(0)
    pass_on(2)
    product(2, 3, 4)
    product(3, 3, 4)
    pass_inner(2)
    pass_next(1)
    for o in range(1, n_t):
        p1r(o).wait_recv()
    total = pb1[0]
    for o in range(1, n_t):
        total = total + pb1[o]
    pb2[dp] = total
    for o in range(1, n_dp):
        p2(o).start()
    pass_next(2)
    for j in range(chunks):
        joined(j, 3)
    pass_on(3)
    for j in range(chunks):
        wcopy(0, j, dp, px).wait_send()
        wcopy(1, j, dp, py).wait_send()
        wcopy(2, j, dp, mate).wait_send()
        wcopy(3, j, px, mate).wait_send()
        wcopy(4, j, py, mate).wait_send()
        wcopy(5, j, px, py, h=0).wait_send()
        wcopy(6, j, py, px, h=1).wait_send()
        wcopy(7, j, dp ^ 6, mate).wait_send()
        for i in range(n_chip):
            to_mate(j, i).wait_send()
        for copy in (d_x, d_y):
            copy(j).wait_send()
    for h in range(2):
        for o in range(n_t - 1):
            split = o == 0 and h == 1

            @pl.when((t - o >= 0) & (t + 1 < n_t - split))
            def _():
                xcopy(0, o, h, t - o, t + 1).wait_send()

            @pl.when((t + o < n_t) & (t > int(split)))
            def _():
                xcopy(1, o, h, t + o, t - 1).wait_send()

    @pl.when(m > 0)
    def _():
        for k in range(2):
            qcopy(k, t, t - sign).wait_send()
        for p in range(parts):
            zcopy(fwd, mirror(n_t - 1), p, t + sign).wait_send()

    @pl.when(m == 0)
    def _():
        for b in (n_t - 1, n_t - 2):
            for p in range(parts):
                zcopy(fwd, mirror(b), p, t + sign).wait_send()
        rb[fwd, t] = jnp.zeros((rows, width), BF16)

    for o in range(1, n_t):
        p1(o).wait_send()
    for j in range(chunks - 1):
        final(j)
    for copy in (x_lo, y_hi, x_hi, y_lo):
        for j in range(chunks - 1):
            copy(j).wait_send()
    for o in range(1, n_dp):
        p2r(o).wait_recv()
    total = pb2[0]
    for o in range(1, n_dp):
        total = total + pb2[o]
    gpre_ref[...] = total[0]
    for o in range(1, n_dp):
        p2(o).wait_send()

    mine = block_rows(t)
    tokens2 = tok_ref[...].astype(F32)
    inv2 = lax.rsqrt(jnp.mean(tokens2 * tokens2, -1, keepdims=True) + EPS)
    dots = jnp.zeros((rows, 1), F32)
    held = []
    for p in range(parts):
        cols = slice(p * tile, (p + 1) * tile)
        zcopy(1 - fwd, t, p, t).wait_recv()

        @pl.when(m > 0)
        def _():
            zcopy(fwd, t, p, t).wait_recv()

        d_normed = (
            dn[mine, cols].astype(F32) + rb[0, t, :, cols].astype(F32) + rb[1, t, :, cols].astype(F32)
        )
        unit = tok_ref[:, cols].astype(F32) * inv2
        e = d_normed * gain_ref[cols][None, :]
        dots = dots + jnp.sum(e * unit, -1, keepdims=True)
        held.append((cols, unit, e))
    mean = dots / width
    for cols, unit, e in held:
        gtok_ref[:, cols] = (inv2 * (e - unit * mean)).astype(BF16)
    final(chunks - 1)

    for copy in (x_lo, y_hi, x_hi, y_lo):
        copy(chunks - 1).wait_send()
    for p in range(parts):

        @pl.when(m == 0)
        def _():
            zcopy(fwd, mirror(1), p, t + sign).wait_send()

        @pl.when(m > 0)
        def _():
            zcopy(fwd, mirror(n_t - 2), p, t + sign).wait_send()
            zcopy(1 - fwd, mirror(0), p, t - sign).wait_send()


def finish_kernel(*refs):
    count = len(refs) // 2
    sems = refs[-1]
    copies = [
        pltpu.make_async_copy(refs[i], refs[count + i], sems.at[i]) for i in range(count)
    ]
    for copy in copies:
        copy.start()
    for copy in copies:
        copy.wait()


def fused_per_device(tokens, cotangent, pre_gain, w_query, key_weight, value_weight):
    n_dp, n_t = lax.axis_size("dp"), lax.axis_size("tensor")
    rows, width = tokens.shape
    block = rows * n_t
    shard = w_query.shape[0]
    chunks = key_weight.shape[1] // HEAD_SIZE
    rep = w_query.shape[1] // key_weight.shape[1]
    qw = rep * HEAD_SIZE
    cw = qw + 2 * HEAD_SIZE
    kw = chunks * HEAD_SIZE
    half = HEAD_SIZE // 2
    parts = 3 if width % (3 * HEAD_SIZE) == 0 else 1
    n_chip = n_dp // 2
    place = np.arange(rows)
    freqs = BASE ** (-np.arange(half) / half)
    angles = (place % SEQ_LEN)[:, None] * freqs[None, :]
    cosine = np.concatenate([np.cos(angles)] * 2, -1).astype(np.float32)
    sine = np.concatenate([-np.sin(angles), np.sin(angles)], -1).astype(np.float32)
    mask = (place[None, :] <= place[:, None]) & (
        place[None, :] // SEQ_LEN == place[:, None] // SEQ_LEN
    )
    mask = np.tile(mask.astype(np.float32), (rep, 1))
    vmem = pl.BlockSpec(memory_space=pltpu.VMEM)
    hbm = pl.BlockSpec(memory_space=pl.ANY)
    dma = pltpu.SemaphoreType.DMA
    made = pl.pallas_call(
        functools.partial(whole_kernel, (n_dp, n_t, chunks, rep, HEAD_SIZE, width // parts)),
        out_shape=(
            pltpu.VMEM((block, chunks * qw), BF16),
            pltpu.VMEM((rows, width), BF16),
            pltpu.VMEM((shard, chunks * qw), F32),
            pltpu.VMEM((shard, kw), F32),
            pltpu.VMEM((shard, kw), F32),
            pltpu.VMEM((width,), F32),
        ),
        in_specs=[hbm] * 9,
        out_specs=(vmem,) * 6,
        scratch_shapes=[
            pltpu.VMEM((rows, width), BF16),
            pltpu.VMEM((width,), F32),
            pltpu.VMEM((block, chunks * qw), BF16),
            pltpu.VMEM(cosine.shape, F32),
            pltpu.VMEM(sine.shape, F32),
            pltpu.VMEM(mask.shape, F32),
            pltpu.VMEM((block, width), BF16),
            pltpu.VMEM((width, block), BF16),
            pltpu.VMEM((chunks, width, cw), BF16),
            pltpu.VMEM((chunks, cw, width), BF16),
            pltpu.VMEM((3, rows, cw), F32),
            pltpu.VMEM((chunks, block, cw), BF16),
            pltpu.VMEM((chunks, n_chip, 2, shard, cw), BF16),
            pltpu.VMEM((chunks, n_chip, shard, cw), BF16),
            pltpu.VMEM((chunks, shard, cw), BF16),
            pltpu.VMEM((2, chunks, shard, cw), BF16),
            pltpu.VMEM((block, width), BF16),
            pltpu.VMEM((2, n_t, rows, width), BF16),
            pltpu.VMEM((n_t, 1, width), F32),
            pltpu.VMEM((n_dp, 1, width), F32),
            dma((8, chunks)),
            dma((8, chunks)),
            dma((2, n_t, 2)),
            dma((2, n_t, 2)),
            dma((2,)),
            dma((2,)),
            dma((chunks, n_chip)),
            dma((chunks, n_chip)),
            dma((6, chunks)),
            dma((6, chunks)),
            dma((2, n_t, parts)),
            dma((2, n_t, parts)),
            dma((2, n_dp)),
            dma((2, n_dp)),
            dma((3, chunks)),
            dma((6,)),
        ],
        compiler_params=pltpu.CompilerParams(
            collective_id=0, has_side_effects=True, vmem_limit_bytes=57 * 1024 * 1024
        ),
    )(tokens, pre_gain, w_query, key_weight, value_weight, cotangent, cosine, sine, mask)
    return pl.pallas_call(
        finish_kernel,
        out_shape=(
            jax.ShapeDtypeStruct((block, chunks * qw), BF16),
            jax.ShapeDtypeStruct((rows, width), BF16),
            jax.ShapeDtypeStruct((shard, chunks * qw), F32),
            jax.ShapeDtypeStruct((shard, kw), F32),
            jax.ShapeDtypeStruct((shard, kw), F32),
            jax.ShapeDtypeStruct((width,), F32),
        ),
        in_specs=[vmem] * 6,
        out_specs=(hbm,) * 6,
        scratch_shapes=[
            dma((6,)),
        ],
        compiler_params=pltpu.CompilerParams(vmem_limit_bytes=16 * 1024 * 1024),
    )(*made)


def solution(mesh):
    fused = mesh.shape["dp"] == 8 and mesh.shape["tensor"] == 4
    placed = (
        P(("dp", "tensor"), None),
        P("dp", "tensor"),
        P(),
        P("dp", "tensor"),
        P("dp", "tensor"),
        P("dp", "tensor"),
    )
    return jax.shard_map(
        fused_per_device if fused else per_device,
        mesh=mesh,
        in_specs=placed,
        out_specs=(
            P("dp", "tensor"),
            P(("dp", "tensor"), None),
            P("dp", "tensor"),
            P("dp", "tensor"),
            P("dp", "tensor"),
            P(),
        ),
        check_vma=False,
    )
```

```python
import functools

import jax
import jax.numpy as jnp
import numpy as np
from jax import lax
from jax.experimental import pallas as pl
from jax.experimental.pallas import tpu as pltpu
from jax.sharding import PartitionSpec as P

HEAD_SIZE = 128
SEQ_LEN = 64


EPS = 1e-06
CAP = 50.0
BASE = 10000.0
query_scalar = 144.0


def rotary_tables(segment_length, half):
    places = jnp.arange(segment_length, dtype=jnp.float32)[:, None]
    freqs = BASE ** (-jnp.arange(half, dtype=jnp.float32) / half)
    angles = places * freqs[None, :]
    return (jnp.cos(angles)[:, None, :], jnp.sin(angles)[:, None, :])


def rotate(values, cosine_table, sine_table):
    half = values.shape[-1] // 2
    first, second = (values[..., :half], values[..., half:])
    return jnp.concatenate(
        [first * cosine_table - second * sine_table, second * cosine_table + first * sine_table], -1
    )


def inverse_rotation(values, cosine_table, sine_table):
    half = values.shape[-1] // 2
    first, second = (values[..., :half], values[..., half:])
    return jnp.concatenate(
        [first * cosine_table + second * sine_table, second * cosine_table - first * sine_table], -1
    )


def attend_forward(query, key, value):
    repeat = query.shape[1] // key.shape[1]
    keys = jnp.repeat(key, repeat, axis=1)
    values = jnp.repeat(value, repeat, axis=1)
    factor = query_scalar ** (-0.5)
    raw = jnp.einsum("qhd,khd->hqk", query, keys, preferred_element_type=jnp.float32) * factor
    bent = jnp.tanh(raw / CAP)
    capped = CAP * bent
    segment_length = query.shape[0]
    causal = jnp.arange(segment_length)[None, :] <= jnp.arange(segment_length)[:, None]
    raised = jnp.where(causal[None], jnp.exp(capped), 0.0)
    weights = raised / jnp.sum(raised, -1, keepdims=True)
    probs = weights.astype(jnp.bfloat16)
    attended = jnp.einsum("hqk,khd->qhd", probs, values, preferred_element_type=jnp.float32).astype(
        jnp.bfloat16
    )
    return (attended, weights, probs, bent)


def attend_backward(d_attended, query, key, value, weights, probs, bent):
    repeat = query.shape[1] // key.shape[1]
    keys = jnp.repeat(key, repeat, axis=1)
    values = jnp.repeat(value, repeat, axis=1)
    factor = query_scalar ** (-0.5)
    d_probs = jnp.einsum("qhd,khd->hqk", d_attended, values, preferred_element_type=jnp.float32)
    d_capped = weights * (d_probs - jnp.sum(weights * d_probs, -1, keepdims=True))
    d_scores = (d_capped * (1.0 - bent * bent) * factor).astype(jnp.bfloat16)
    query_back = jnp.einsum("hqk,khd->qhd", d_scores, keys, preferred_element_type=jnp.float32)
    key_heads = jnp.einsum("hqk,qhd->khd", d_scores, query, preferred_element_type=jnp.float32)
    value_heads = jnp.einsum("hqk,qhd->khd", probs, d_attended, preferred_element_type=jnp.float32)
    segment_length, heads, width = query.shape
    key_rotated_back = key_heads.reshape(segment_length, heads // repeat, repeat, width).sum(2)
    value_returned = value_heads.reshape(segment_length, heads // repeat, repeat, width).sum(2)
    return (query_back, key_rotated_back, value_returned)


def segment_pass(query, key, value, d_attended):
    attended, weights, probs, bent = attend_forward(query, key, value)
    query_back, key_rotated_back, value_returned = attend_backward(
        d_attended, query, key, value, weights, probs, bent
    )
    return (attended, query_back, key_rotated_back, value_returned)


def per_device(tokens, cotangent, pre_gain, w_query, key_weight, value_weight):
    contract_first = (((0,), (0,)), ((), ()))
    contract_last = (((1,), (1,)), ((), ()))
    rows_f = tokens.astype(jnp.float32)
    inv_one = lax.rsqrt(jnp.mean(rows_f * rows_f, -1, keepdims=True) + EPS)
    unit_one = rows_f * inv_one
    normed_input = (unit_one * pre_gain).astype(jnp.bfloat16)
    gathered = lax.all_gather(normed_input, "tensor", axis=0, tiled=True)
    segment_length = gathered.shape[0]
    token_span = SEQ_LEN
    pieces_count = segment_length // token_span
    heads_query = w_query.shape[1] // HEAD_SIZE
    heads_key = key_weight.shape[1] // HEAD_SIZE
    pieces = (
        lax.all_gather(w_query, "dp", axis=0, tiled=True),
        lax.all_gather(key_weight, "dp", axis=0, tiled=True),
        lax.all_gather(value_weight, "dp", axis=0, tiled=True),
    )
    query_raw, key_unrotated, value_projected = tuple(
        (jnp.dot(gathered, piece, preferred_element_type=jnp.float32) for piece in pieces)
    )
    cosine_table, sine_table = rotary_tables(token_span, HEAD_SIZE // 2)
    query = rotate(
        query_raw.reshape(pieces_count, token_span, heads_query, HEAD_SIZE),
        cosine_table,
        sine_table,
    ).astype(jnp.bfloat16)
    key = rotate(
        key_unrotated.reshape(pieces_count, token_span, heads_key, HEAD_SIZE),
        cosine_table,
        sine_table,
    ).astype(jnp.bfloat16)
    value = value_projected.reshape(pieces_count, token_span, heads_key, HEAD_SIZE).astype(
        jnp.bfloat16
    )
    d_attended = cotangent.reshape(pieces_count, token_span, heads_query, HEAD_SIZE)
    attended, query_back, key_rotated_back, value_returned = jax.vmap(segment_pass)(
        query, key, value, d_attended
    )
    attended_flat = attended.reshape(segment_length, heads_query * HEAD_SIZE)
    d_query = (
        inverse_rotation(query_back, cosine_table, sine_table)
        .astype(jnp.bfloat16)
        .reshape(segment_length, heads_query * HEAD_SIZE)
    )
    key_gradient = (
        inverse_rotation(key_rotated_back, cosine_table, sine_table)
        .astype(jnp.bfloat16)
        .reshape(segment_length, heads_key * HEAD_SIZE)
    )
    value_gradient = value_returned.astype(jnp.bfloat16).reshape(
        segment_length, heads_key * HEAD_SIZE
    )
    back_query, back_key, back_value = (
        lax.all_gather(w_query, "dp", axis=0, tiled=True),
        lax.all_gather(key_weight, "dp", axis=0, tiled=True),
        lax.all_gather(value_weight, "dp", axis=0, tiled=True),
    )
    joined = jnp.concatenate([d_query, key_gradient, value_gradient], 1)
    block = gathered
    grads = lax.psum_scatter(
        lax.dot_general(block, joined, contract_first, preferred_element_type=jnp.float32).astype(
            jnp.bfloat16
        ),
        "dp",
        scatter_dimension=0,
        tiled=True,
    ).astype(jnp.float32)
    width_query = w_query.shape[1]
    width_key = key_weight.shape[1]
    grad_query = grads[:, :width_query]
    grad_key = grads[:, width_query : width_query + width_key]
    grad_value = grads[:, width_query + width_key :]
    total = jnp.zeros((tokens.shape[0] * lax.axis_size("tensor"), gathered.shape[1]), jnp.float32)
    for grad_part, weight in (
        (d_query, back_query),
        (key_gradient, back_key),
        (value_gradient, back_value),
    ):
        block = grad_part
        total = total + lax.dot_general(
            block, weight, contract_last, preferred_element_type=jnp.float32
        )
    d_normed = lax.psum_scatter(
        total.astype(jnp.bfloat16), "tensor", scatter_dimension=0, tiled=True
    ).astype(jnp.float32)
    pre_part = jnp.sum(d_normed * unit_one, 0)
    scaled_in = d_normed * pre_gain
    grad_tokens = (
        inv_one * (scaled_in - unit_one * jnp.mean(scaled_in * unit_one, -1, keepdims=True))
    ).astype(jnp.bfloat16)
    grad_pre = lax.psum(pre_part, ("dp", "tensor"))
    return (attended_flat, grad_tokens, grad_query, grad_key, grad_value, grad_pre)


F32 = jnp.float32
BF16 = jnp.bfloat16
NN = (((1,), (0,)), ((), ()))
NT = (((1,), (1,)), ((), ()))
TN = (((0,), (0,)), ((), ()))


def swap_halves(values):
    half = values.shape[-1] // 2
    return jnp.concatenate([values[:, half:], values[:, :half]], -1)


W_SLOT = (0, 1, 2, 2, 2, 3, 3, 2)


def whole_kernel(
    dims,
    tok_hbm,
    gain_hbm,
    wq_ref,
    wk_ref,
    wv_ref,
    cot_hbm,
    cos_hbm,
    sin_hbm,
    mask_hbm,
    att_ref,
    gtok_ref,
    gq_ref,
    gk_ref,
    gv_ref,
    gpre_ref,
    tok_ref,
    gain_ref,
    cot_ref,
    cos_ref,
    sin_ref,
    mask_ref,
    x,
    xt,
    w,
    wt,
    proj,
    dproj,
    g,
    pr,
    dr,
    ar,
    dn,
    rb,
    pb1,
    pb2,
    ws,
    wr,
    xs,
    xr,
    qr,
    ms,
    mr,
    gs,
    gr,
    zs,
    zr,
    ps,
    prs,
    ls,
    ins,
):
    n_dp, n_t, chunks, rep, hd, tile = dims
    dp = lax.axis_index("dp")
    t = lax.axis_index("tensor")
    rows = tok_ref.shape[0]
    width = tok_ref.shape[1]
    shard = wq_ref.shape[0]
    qw = rep * hd
    cw = qw + 2 * hd
    half = shard // 2
    n_chip = n_dp // 2
    parts = width // tile
    core = lax.rem(dp, 2)
    chip = lax.div(dp, 2)
    mate, px, py = dp ^ 1, dp ^ 2, dp ^ 4

    barrier = pltpu.get_barrier_semaphore()

    def greet(d, z):
        pl.semaphore_signal(
            barrier, inc=1, device_id=(d, z), device_id_type=pl.DeviceIdType.MESH
        )

    greet(px, t)
    greet(py, t)

    @pl.when(t < n_t - 1)
    def _():
        greet(dp, t + 1)

    @pl.when(t > 0)
    def _():
        greet(dp, t - 1)

    greet(mate, t)

    loads = [
        pltpu.make_async_copy(src, dst, ins.at[i])
        for i, (src, dst) in enumerate(
            (
                (tok_hbm, tok_ref),
                (gain_hbm, gain_ref),
                (cos_hbm, cos_ref),
                (sin_hbm, sin_ref),
                (mask_hbm, mask_ref),
                (cot_hbm, cot_ref),
            )
        )
    ]

    def own_copies(j):
        here = pl.ds(pl.multiple_of(dp * shard, 16), shard)
        return (
            pltpu.make_async_copy(
                wq_ref.at[:, j * qw : (j + 1) * qw], w.at[j, here, 0:qw], ls.at[j]
            ),
            pltpu.make_async_copy(
                wk_ref.at[:, j * hd : (j + 1) * hd], w.at[j, here, qw : qw + hd], ls.at[j]
            ),
            pltpu.make_async_copy(
                wv_ref.at[:, j * hd : (j + 1) * hd], w.at[j, here, qw + hd : cw], ls.at[j]
            ),
        )

    def own_wait(j):
        here = pl.ds(pl.multiple_of(dp * shard, 16), shard)
        pltpu.make_async_copy(wq_ref.at[:, 0:cw], w.at[j, here], ls.at[j]).wait()

    loads[0].start()
    loads[1].start()
    for j in range(chunks):
        for copy in own_copies(j):
            copy.start()
    for copy in loads[2:]:
        copy.start()

    def rdma(src, dst, ssem, rsem, d, z):
        return pltpu.make_async_remote_copy(
            src_ref=src,
            dst_ref=dst,
            send_sem=ssem,
            recv_sem=rsem,
            device_id=(d, z),
            device_id_type=pl.DeviceIdType.MESH,
        )

    def wrow(who, h=None):
        if h is None:
            return pl.ds(pl.multiple_of(who * shard, 16), shard)
        return pl.ds(pl.multiple_of(who * shard + h * half, 16), half)

    def wcopy(kind, j, origin, to, h=None):
        place = w.at[j, wrow(origin, h)]
        return rdma(place, place, ws.at[j], wr.at[W_SLOT[kind], j], to, t)

    def whole(count, j, slot):
        place = w.at[j, 0 : count * shard]
        return rdma(place, place, ws.at[j], wr.at[slot, j], mate, t)

    def offer(j):
        wcopy(0, j, dp, px).start()
        wcopy(1, j, dp, py).start()

    low = t < n_t // 2
    sign = jnp.where(low, 1, -1)
    m = jnp.where(low, t, n_t - 1 - t)
    fwd = jnp.where(low, 0, 1)
    piece, quarter = rows // 2, rows // 4
    mine_next = t + sign

    def xcopy(way, o, h, origin, to):
        place = x.at[pl.ds(pl.multiple_of(origin * rows + h * piece, piece), piece)]
        return rdma(place, place, xs.at[min(o, 1)], xr.at[way, o, h], dp, to)

    def xpart(origin, count, k):
        place = x.at[pl.ds(pl.multiple_of(origin * rows, rows), count)]
        return rdma(place, place, xs.at[k], qr.at[0], dp, mine_next)

    def qcopy(k, origin, to):
        first = pl.multiple_of(origin * rows + piece + k * quarter, quarter)
        place = x.at[pl.ds(first, quarter)]
        return rdma(place, place, xs.at[0], qr.at[0], dp, to)

    own_wait(0)
    pl.semaphore_wait(barrier, 3 + jnp.where(m == 0, 1, 2))
    offer(0)
    own_wait(1)
    offer(1)
    loads[0].wait()
    loads[1].wait()
    tokens = tok_ref[...].astype(F32)
    inv = lax.rsqrt(jnp.mean(tokens * tokens, -1, keepdims=True) + EPS)
    x[pl.ds(pl.multiple_of(t * rows, rows), rows), :] = (
        (tokens * inv) * gain_ref[...][None, :]
    ).astype(BF16)

    @pl.when(t < n_t - 1)
    def _():
        xcopy(0, 0, 0, t, t + 1).start()

    @pl.when(t > 0)
    def _():
        xcopy(1, 0, 0, t, t - 1).start()

    @pl.when(t < n_t - 2)
    def _():
        xcopy(0, 0, 1, t, t + 1).start()

    @pl.when(t > 1)
    def _():
        xcopy(1, 0, 1, t, t - 1).start()

    @pl.when(m > 0)
    def _():
        qcopy(0, t, t - sign).start()

    for j in range(2, chunks):
        own_wait(j)
    for j in range(chunks):
        wcopy(2, j, dp, mate).start()
    for copy in loads[2:]:
        copy.wait()

    def relay(j):
        wcopy(0, j, px, px).wait_recv()
        wcopy(5, j, px, py, h=0).start()
        wcopy(3, j, px, mate).start()
        wcopy(1, j, py, py).wait_recv()
        wcopy(6, j, py, px, h=1).start()
        wcopy(4, j, py, mate).start()

    def xrelay(o, h):
        split = o == 1 and h == 1
        above = (t - o >= 0) & (t < n_t - 1) if split else t - o >= 0
        below = (t + o < n_t) & (t > 0) if split else t + o < n_t

        @pl.when(above)
        def _():
            xcopy(0, o - 1, h, t - o, t).wait_recv()

            @pl.when(t + 1 < n_t)
            def _():
                xcopy(0, o, h, t - o, t + 1).start()

        @pl.when(below)
        def _():
            xcopy(1, o - 1, h, t + o, t).wait_recv()

            @pl.when(t > 0)
            def _():
                xcopy(1, o, h, t + o, t - 1).start()

    def xlate():
        @pl.when(m > 0)
        def _():
            qcopy(1, t, t - sign).start()

    def xfinish():
        @pl.when(m == 0)
        def _():
            xpart(t + sign, piece, 0).wait_recv()

    def far(j):
        whole(1, j, 3).wait_recv()
        wcopy(7, j, dp ^ 6, mate).start()

    def ready(j, relayed=False):
        if not relayed:
            far(j)
        whole(n_chip, j, 2).wait_recv()

    factor = query_scalar ** (-0.5)

    def mirror(b):
        return jnp.where(low, b, n_t - 1 - b)

    places = (
        t,
        jnp.where(m == 0, t + sign, t - sign),
        jnp.where(m == 0, t + 2 * sign, t + sign),
        mirror(n_t - 1),
    )

    def head_cols(j, i):
        return pl.ds(pl.multiple_of(j * qw + i * hd, hd), hd)

    def block_rows(b, count=1):
        return pl.ds(pl.multiple_of(b * rows, rows), count * rows)

    def tiles(*which):
        for slot, (j, p) in enumerate(which):
            here = block_rows(places[p])
            proj[slot] = lax.dot_general(x[here, :], w[j], NN, preferred_element_type=F32)
        for slot, (j, p) in enumerate(which):
            here = block_rows(places[p])
            cosv, sinv = cos_ref[...], sin_ref[...]

            def turn(v):
                return v * cosv + swap_halves(v) * sinv

            def unturn(v):
                return v * cosv - swap_halves(v) * sinv

            q = jnp.concatenate(
                [turn(proj[slot, :, i * hd : (i + 1) * hd]).astype(BF16) for i in range(rep)], 0
            )
            k = turn(proj[slot, :, qw : qw + hd]).astype(BF16)
            v = proj[slot, :, qw + hd : cw].astype(BF16)
            cot = jnp.concatenate(
                [cot_ref[here, head_cols(j, i)] for i in range(rep)], 0
            )
            bent = jnp.tanh(
                lax.dot_general(q, k, NT, preferred_element_type=F32) * factor / CAP
            )
            raised = jnp.exp(CAP * bent) * mask_ref[...]
            weights = raised / jnp.sum(raised, -1, keepdims=True)
            probs = weights.astype(BF16)
            att = lax.dot_general(probs, v, NN, preferred_element_type=F32).astype(BF16)
            d_probs = lax.dot_general(cot, v, NT, preferred_element_type=F32)
            d_capped = weights * (d_probs - jnp.sum(weights * d_probs, -1, keepdims=True))
            ds = (d_capped * (1.0 - bent * bent) * factor).astype(BF16)
            dq = lax.dot_general(ds, k, NN, preferred_element_type=F32)
            dk = lax.dot_general(ds, q, TN, preferred_element_type=F32)
            dv = lax.dot_general(probs, cot, TN, preferred_element_type=F32)
            for i in range(rep):
                part = slice(i * rows, (i + 1) * rows)
                att_ref[here, head_cols(j, i)] = att[part]
                dproj[j, here, i * hd : (i + 1) * hd] = unturn(dq[part]).astype(BF16)
            dproj[j, here, qw : qw + hd] = unturn(dk).astype(BF16)
            dproj[j, here, qw + hd : cw] = dv.astype(BF16)

    def flip_rows(p):
        here = block_rows(places[p])
        xt[:, here] = x[here, :].T

    def flip_weights(j):
        wt[j] = w[j].T

    def span(p):
        return pl.ds(pl.multiple_of(p * tile, tile), tile)

    def zcopy(way, b, p, to):
        return rdma(
            dn.at[block_rows(b), span(p)],
            rb.at[way, b, :, span(p)],
            zs.at[0],
            zr.at[way, b, p],
            dp,
            to,
        )

    def outward(b, p):
        zcopy(fwd, mirror(b), p, t + sign).start()

    def back(first, count, sent=None):
        here = block_rows(first, count)

        def cols(p, c2):
            total = lax.dot_general(
                dproj[0, here, :], wt[0, :, span(p)], NN, preferred_element_type=F32
            )
            for j in range(1, chunks):
                total += lax.dot_general(
                    dproj[j, here, :], wt[j, :, span(p)], NN, preferred_element_type=F32
                )
            dn[here, span(p)] = total.astype(BF16)

            if sent is not None:

                @pl.when(m == 0)
                def _():
                    outward(sent, p)

            return c2

        lax.fori_loop(0, parts, cols, 0)

    strip = 64

    def gain_part(first, count, fresh):
        def cols(p, c2):
            def step(r, acc):
                here = pl.ds(pl.multiple_of(first * rows + r * strip, strip), strip)
                both = dn[here, span(p)].astype(F32) * x[here, span(p)].astype(F32)
                return acc + jnp.sum(both.reshape(strip // 8, 8, tile), 0)

            acc = lax.fori_loop(0, count * rows // strip, step, jnp.zeros((8, tile), F32))
            total = jnp.sum(acc, 0, keepdims=True)
            if not fresh:
                total = total + pb1[t, :, span(p)]
            pb1[t, :, span(p)] = total
            return c2

        lax.fori_loop(0, parts, cols, 0)

    lo, hi = pl.ds(0, half), pl.ds(half, half)

    def to_mate(j, i):
        return rdma(g.at[j, i, 0], pr.at[j, i], ms.at[j], mr.at[j, i], mate, t)

    def gcopy(kind, j, src, dst, to):
        return rdma(src, dst, gs.at[j], gr.at[min(kind, 2), j], to, t)

    def d_x(j):
        return gcopy(0, j, pr.at[j, 0, lo], dr.at[j, lo], px)

    def d_y(j):
        return gcopy(1, j, pr.at[j, 0, hi], dr.at[j, hi], py)

    def x_lo(j):
        return gcopy(2, j, pr.at[j, 2, lo], ar.at[0, j, lo], px)

    def x_hi(j):
        return gcopy(3, j, pr.at[j, 2, hi], ar.at[0, j, hi], px)

    def y_lo(j):
        return gcopy(4, j, pr.at[j, 1, lo], ar.at[1, j, lo], py)

    def y_hi(j):
        return gcopy(5, j, pr.at[j, 1, hi], ar.at[1, j, hi], py)

    def add(*terms):
        total = terms[0].astype(F32)
        for term in terms[1:]:
            total = total + term.astype(F32)
        return total.astype(BF16)

    def product(j, first=0, last=n_chip):
        def share(i, c2):
            c = chip ^ (n_chip - 1 - i)
            for k, who in enumerate((2 * c + 1 - core, 2 * c + core)):
                here = pl.ds(pl.multiple_of(who * shard, 16), shard)
                g[j, i, k] = lax.dot_general(
                    xt[here, :], dproj[j], NN, preferred_element_type=F32
                ).astype(BF16)
                if k == 0:
                    to_mate(j, i).start()
            return c2

        lax.fori_loop(first, last, share, 0)

    def joined(j, i):
        to_mate(j, i).wait_recv()
        pr[j, i] = add(g[j, i, 1], pr[j, i])

    def on_chip_far(j):
        joined(j, 0)
        d_x(j).start()
        d_y(j).start()

    def on_chip_near(j):
        joined(j, 1)
        y_hi(j).start()
        joined(j, 2)
        x_lo(j).start()

    def pass_on(j):
        d_x(j).wait_recv()
        pr[j, 1, lo] = add(pr[j, 1, lo], dr[j, lo])
        y_lo(j).start()
        d_y(j).wait_recv()
        pr[j, 2, hi] = add(pr[j, 2, hi], dr[j, hi])
        x_hi(j).start()

    def zsum(way, b, p):
        here = block_rows(b)
        cols = slice(p * tile, (p + 1) * tile)
        zcopy(way, b, p, t).wait_recv()
        dn[here, cols] = add(dn[here, cols], rb[way, b, :, cols])

    far_block = mirror(n_t - 1)
    rest = jnp.where(low, 0, 1)
    near_pair = jnp.where(low, 0, n_t - 2)

    def pass_far(p):
        @pl.when(m > 0)
        def _():
            zsum(fwd, far_block, p)
            outward(n_t - 1, p)

    def pass_inner(p):
        @pl.when(m > 0)
        def _():
            zsum(1 - fwd, mirror(0), p)
            zcopy(1 - fwd, mirror(0), p, t - sign).start()

    def pass_next(p):
        @pl.when(m > 0)
        def _():
            zsum(fwd, mirror(n_t - 2), p)
            outward(n_t - 2, p)

    def p1(o):
        return rdma(pb1.at[t], pb1.at[t], ps.at[0], prs.at[0], dp, t ^ o)

    def p2(o):
        return rdma(pb2.at[dp], pb2.at[dp], ps.at[1], prs.at[1], dp ^ o, t)

    def p1_all():
        place = pb1.at[0 : n_t - 1]
        return rdma(place, place, ps.at[0], prs.at[0], dp, mine_next)

    def p2_all():
        place = pb2.at[0 : n_dp - 1]
        return rdma(place, place, ps.at[1], prs.at[1], mate, t)

    def final(j):
        gcopy(2, j, pr.at[j, 0:2], ar.at[:, j], px).wait_recv()
        done = pr[j, 3].astype(F32) + ar[0, j].astype(F32) + ar[1, j].astype(F32)
        gq_ref[:, j * qw : (j + 1) * qw] = done[:, :qw]
        gk_ref[:, j * hd : (j + 1) * hd] = done[:, qw : qw + hd]
        gv_ref[:, j * hd : (j + 1) * hd] = done[:, qw + hd :]

    relay(0)
    offer(2)
    xrelay(1, 0)
    flip_rows(0)
    relay(1)
    offer(3)
    xrelay(1, 1)
    ready(0)
    tiles((0, 0))
    xrelay(2, 0)
    relay(2)
    flip_weights(0)
    far(1)
    xrelay(2, 1)
    xlate()
    ready(1, True)
    tiles((1, 0), (0, 2), (1, 2))
    flip_rows(2)
    relay(3)
    flip_weights(1)
    xrelay(3, 0)
    xrelay(3, 1)
    tiles((0, 3), (1, 3))
    far(2)
    flip_rows(3)
    ready(2, True)
    xfinish()
    far(3)
    tiles((0, 1), (2, 3))
    flip_rows(1)
    product(0, 0, 1)
    ready(3, True)
    tiles((3, 3))
    on_chip_far(0)
    flip_weights(2)
    flip_weights(3)
    back(far_block, 1, n_t - 1)
    gain_part(far_block, 1, True)
    product(0, 1, 3)
    tiles((1, 1))
    on_chip_near(0)
    pass_on(0)
    product(1, 0, 3)
    pass_far(0)
    on_chip_far(1)
    tiles((2, 2), (3, 2))
    on_chip_near(1)
    back(mirror(n_t - 2), 1, n_t - 2)
    pass_far(1)
    tiles((2, 0), (2, 1))
    product(2, 0, 1)
    tiles((3, 0), (3, 1))
    on_chip_far(2)
    pass_far(2)
    back(near_pair, 2)
    pass_on(1)
    gain_part(rest, n_t - 1, False)
    pb1[t] = pb1[t] / gain_ref[...][None, :]
    for o in range(1, n_t):
        p1(o).start()

    @pl.when(m == 0)
    def _():
        for p in range(parts):
            outward(1, p)

    product(2, 1, 3)
    product(3, 0, 3)
    on_chip_near(2)
    pass_inner(0)
    on_chip_far(3)
    product(0, 3, 4)
    product(1, 3, 4)
    on_chip_near(3)
    pass_on(2)
    pass_inner(1)
    pass_next(0)
    product(2, 3, 4)
    product(3, 3, 4)
    pass_inner(2)
    pass_next(1)
    p1_all().wait_recv()
    total = pb1[0]
    for o in range(1, n_t):
        total = total + pb1[o]
    pb2[dp] = total
    for o in range(1, n_dp):
        p2(o).start()
    pass_next(2)
    for j in range(chunks):
        joined(j, 3)
    pass_on(3)
    for j in range(chunks):
        whole(n_dp - 1, j, 2).wait_send()
        rdma(g.at[j, :, 0], pr.at[j], ms.at[j], mr.at[j, 0], mate, t).wait_send()

    @pl.when(m == 0)
    def _():
        xpart(0, rows, 0).wait_send()
        rb[fwd, t] = jnp.zeros((rows, width), BF16)

    @pl.when(m > 0)
    def _():
        xpart(0, 2 * rows, 0).wait_send()
        xpart(0, (n_t - 1) * rows, 1).wait_send()

    p1_all().wait_send()
    for j in range(chunks - 1):
        final(j)
        gcopy(2, j, pr.at[j, 0:3], pr.at[j, 0:3], px).wait_send()
    p2_all().wait_recv()
    total = pb2[0]
    for o in range(1, n_dp):
        total = total + pb2[o]
    gpre_ref[...] = total[0]
    p2_all().wait_send()

    mine = block_rows(t)
    tokens2 = tok_ref[...].astype(F32)
    inv2 = lax.rsqrt(jnp.mean(tokens2 * tokens2, -1, keepdims=True) + EPS)
    dots = jnp.zeros((rows, 1), F32)
    held = []
    for p in range(parts):
        cols = slice(p * tile, (p + 1) * tile)
        zcopy(1 - fwd, t, p, t).wait_recv()

        @pl.when(m > 0)
        def _():
            zcopy(fwd, t, p, t).wait_recv()

        d_normed = (
            dn[mine, cols].astype(F32) + rb[0, t, :, cols].astype(F32) + rb[1, t, :, cols].astype(F32)
        )
        unit = tok_ref[:, cols].astype(F32) * inv2
        e = d_normed * gain_ref[cols][None, :]
        dots = dots + jnp.sum(e * unit, -1, keepdims=True)
        held.append((cols, unit, e))
    mean = dots / width
    for cols, unit, e in held:
        gtok_ref[:, cols] = (inv2 * (e - unit * mean)).astype(BF16)
    final(chunks - 1)

    gcopy(2, chunks - 1, pr.at[chunks - 1, 0:3], pr.at[chunks - 1, 0:3], px).wait_send()
    sent = dn.at[0 : (n_t - 1) * rows]
    rdma(sent, sent, zs.at[0], zr.at[0, 0, 0], dp, mine_next).wait_send()


def finish_kernel(*refs):
    count = len(refs) // 2
    sems = refs[-1]
    copies = [
        pltpu.make_async_copy(refs[i], refs[count + i], sems.at[i]) for i in range(count)
    ]
    for copy in copies:
        copy.start()
    for copy in copies:
        copy.wait()


def fused_per_device(tokens, cotangent, pre_gain, w_query, key_weight, value_weight):
    n_dp, n_t = lax.axis_size("dp"), lax.axis_size("tensor")
    rows, width = tokens.shape
    block = rows * n_t
    shard = w_query.shape[0]
    chunks = key_weight.shape[1] // HEAD_SIZE
    rep = w_query.shape[1] // key_weight.shape[1]
    qw = rep * HEAD_SIZE
    cw = qw + 2 * HEAD_SIZE
    kw = chunks * HEAD_SIZE
    half = HEAD_SIZE // 2
    parts = 3 if width % (3 * HEAD_SIZE) == 0 else 1
    n_chip = n_dp // 2
    place = np.arange(rows)
    freqs = BASE ** (-np.arange(half) / half)
    angles = (place % SEQ_LEN)[:, None] * freqs[None, :]
    cosine = np.concatenate([np.cos(angles)] * 2, -1).astype(np.float32)
    sine = np.concatenate([-np.sin(angles), np.sin(angles)], -1).astype(np.float32)
    mask = (place[None, :] <= place[:, None]) & (
        place[None, :] // SEQ_LEN == place[:, None] // SEQ_LEN
    )
    mask = np.tile(mask.astype(np.float32), (rep, 1))
    vmem = pl.BlockSpec(memory_space=pltpu.VMEM)
    hbm = pl.BlockSpec(memory_space=pl.ANY)
    dma = pltpu.SemaphoreType.DMA
    made = pl.pallas_call(
        functools.partial(whole_kernel, (n_dp, n_t, chunks, rep, HEAD_SIZE, width // parts)),
        out_shape=(
            pltpu.VMEM((block, chunks * qw), BF16),
            pltpu.VMEM((rows, width), BF16),
            pltpu.VMEM((shard, chunks * qw), F32),
            pltpu.VMEM((shard, kw), F32),
            pltpu.VMEM((shard, kw), F32),
            pltpu.VMEM((width,), F32),
        ),
        in_specs=[hbm] * 9,
        out_specs=(vmem,) * 6,
        scratch_shapes=[
            pltpu.VMEM((rows, width), BF16),
            pltpu.VMEM((width,), F32),
            pltpu.VMEM((block, chunks * qw), BF16),
            pltpu.VMEM(cosine.shape, F32),
            pltpu.VMEM(sine.shape, F32),
            pltpu.VMEM(mask.shape, F32),
            pltpu.VMEM((block, width), BF16),
            pltpu.VMEM((width, block), BF16),
            pltpu.VMEM((chunks, width, cw), BF16),
            pltpu.VMEM((chunks, cw, width), BF16),
            pltpu.VMEM((4, rows, cw), F32),
            pltpu.VMEM((chunks, block, cw), BF16),
            pltpu.VMEM((chunks, n_chip, 2, shard, cw), BF16),
            pltpu.VMEM((chunks, n_chip, shard, cw), BF16),
            pltpu.VMEM((chunks, shard, cw), BF16),
            pltpu.VMEM((2, chunks, shard, cw), BF16),
            pltpu.VMEM((block, width), BF16),
            pltpu.VMEM((2, n_t, rows, width), BF16),
            pltpu.VMEM((n_t, 1, width), F32),
            pltpu.VMEM((n_dp, 1, width), F32),
            dma((chunks,)),
            dma((4, chunks)),
            dma((2,)),
            dma((2, n_t - 1, 2)),
            dma((1,)),
            dma((chunks,)),
            dma((chunks, n_chip)),
            dma((chunks,)),
            dma((3, chunks)),
            dma((1,)),
            dma((2, n_t, parts)),
            dma((2,)),
            dma((2,)),
            dma((chunks,)),
            dma((6,)),
        ],
        compiler_params=pltpu.CompilerParams(
            collective_id=0, has_side_effects=True, vmem_limit_bytes=57 * 1024 * 1024
        ),
    )(tokens, pre_gain, w_query, key_weight, value_weight, cotangent, cosine, sine, mask)
    return pl.pallas_call(
        finish_kernel,
        out_shape=(
            jax.ShapeDtypeStruct((block, chunks * qw), BF16),
            jax.ShapeDtypeStruct((rows, width), BF16),
            jax.ShapeDtypeStruct((shard, chunks * qw), F32),
            jax.ShapeDtypeStruct((shard, kw), F32),
            jax.ShapeDtypeStruct((shard, kw), F32),
            jax.ShapeDtypeStruct((width,), F32),
        ),
        in_specs=[vmem] * 6,
        out_specs=(hbm,) * 6,
        scratch_shapes=[
            dma((6,)),
        ],
        compiler_params=pltpu.CompilerParams(vmem_limit_bytes=16 * 1024 * 1024),
    )(*made)


def solution(mesh):
    fused = mesh.shape["dp"] == 8 and mesh.shape["tensor"] == 4
    placed = (
        P(("dp", "tensor"), None),
        P("dp", "tensor"),
        P(),
        P("dp", "tensor"),
        P("dp", "tensor"),
        P("dp", "tensor"),
    )
    return jax.shard_map(
        fused_per_device if fused else per_device,
        mesh=mesh,
        in_specs=placed,
        out_specs=(
            P("dp", "tensor"),
            P(("dp", "tensor"), None),
            P("dp", "tensor"),
            P("dp", "tensor"),
            P("dp", "tensor"),
            P(),
        ),
        check_vma=False,
    )
```

```python
import functools

import jax
import jax.numpy as jnp
import numpy as np
from jax import lax
from jax.experimental import pallas as pl
from jax.experimental.pallas import tpu as pltpu
from jax.sharding import PartitionSpec as P

HEAD_SIZE = 128
SEQ_LEN = 64


EPS = 1e-06
CAP = 50.0
BASE = 10000.0
query_scalar = 144.0


def rotary_tables(segment_length, half):
    places = jnp.arange(segment_length, dtype=jnp.float32)[:, None]
    freqs = BASE ** (-jnp.arange(half, dtype=jnp.float32) / half)
    angles = places * freqs[None, :]
    return (jnp.cos(angles)[:, None, :], jnp.sin(angles)[:, None, :])


def rotate(values, cosine_table, sine_table):
    half = values.shape[-1] // 2
    first, second = (values[..., :half], values[..., half:])
    return jnp.concatenate(
        [first * cosine_table - second * sine_table, second * cosine_table + first * sine_table], -1
    )


def inverse_rotation(values, cosine_table, sine_table):
    half = values.shape[-1] // 2
    first, second = (values[..., :half], values[..., half:])
    return jnp.concatenate(
        [first * cosine_table + second * sine_table, second * cosine_table - first * sine_table], -1
    )


def attend_forward(query, key, value):
    repeat = query.shape[1] // key.shape[1]
    keys = jnp.repeat(key, repeat, axis=1)
    values = jnp.repeat(value, repeat, axis=1)
    factor = query_scalar ** (-0.5)
    raw = jnp.einsum("qhd,khd->hqk", query, keys, preferred_element_type=jnp.float32) * factor
    bent = jnp.tanh(raw / CAP)
    capped = CAP * bent
    segment_length = query.shape[0]
    causal = jnp.arange(segment_length)[None, :] <= jnp.arange(segment_length)[:, None]
    raised = jnp.where(causal[None], jnp.exp(capped), 0.0)
    weights = raised / jnp.sum(raised, -1, keepdims=True)
    probs = weights.astype(jnp.bfloat16)
    attended = jnp.einsum("hqk,khd->qhd", probs, values, preferred_element_type=jnp.float32).astype(
        jnp.bfloat16
    )
    return (attended, weights, probs, bent)


def attend_backward(d_attended, query, key, value, weights, probs, bent):
    repeat = query.shape[1] // key.shape[1]
    keys = jnp.repeat(key, repeat, axis=1)
    values = jnp.repeat(value, repeat, axis=1)
    factor = query_scalar ** (-0.5)
    d_probs = jnp.einsum("qhd,khd->hqk", d_attended, values, preferred_element_type=jnp.float32)
    d_capped = weights * (d_probs - jnp.sum(weights * d_probs, -1, keepdims=True))
    d_scores = (d_capped * (1.0 - bent * bent) * factor).astype(jnp.bfloat16)
    query_back = jnp.einsum("hqk,khd->qhd", d_scores, keys, preferred_element_type=jnp.float32)
    key_heads = jnp.einsum("hqk,qhd->khd", d_scores, query, preferred_element_type=jnp.float32)
    value_heads = jnp.einsum("hqk,qhd->khd", probs, d_attended, preferred_element_type=jnp.float32)
    segment_length, heads, width = query.shape
    key_rotated_back = key_heads.reshape(segment_length, heads // repeat, repeat, width).sum(2)
    value_returned = value_heads.reshape(segment_length, heads // repeat, repeat, width).sum(2)
    return (query_back, key_rotated_back, value_returned)


def segment_pass(query, key, value, d_attended):
    attended, weights, probs, bent = attend_forward(query, key, value)
    query_back, key_rotated_back, value_returned = attend_backward(
        d_attended, query, key, value, weights, probs, bent
    )
    return (attended, query_back, key_rotated_back, value_returned)


def per_device(tokens, cotangent, pre_gain, w_query, key_weight, value_weight):
    contract_first = (((0,), (0,)), ((), ()))
    contract_last = (((1,), (1,)), ((), ()))
    rows_f = tokens.astype(jnp.float32)
    inv_one = lax.rsqrt(jnp.mean(rows_f * rows_f, -1, keepdims=True) + EPS)
    unit_one = rows_f * inv_one
    normed_input = (unit_one * pre_gain).astype(jnp.bfloat16)
    gathered = lax.all_gather(normed_input, "tensor", axis=0, tiled=True)
    segment_length = gathered.shape[0]
    token_span = SEQ_LEN
    pieces_count = segment_length // token_span
    heads_query = w_query.shape[1] // HEAD_SIZE
    heads_key = key_weight.shape[1] // HEAD_SIZE
    pieces = (
        lax.all_gather(w_query, "dp", axis=0, tiled=True),
        lax.all_gather(key_weight, "dp", axis=0, tiled=True),
        lax.all_gather(value_weight, "dp", axis=0, tiled=True),
    )
    query_raw, key_unrotated, value_projected = tuple(
        (jnp.dot(gathered, piece, preferred_element_type=jnp.float32) for piece in pieces)
    )
    cosine_table, sine_table = rotary_tables(token_span, HEAD_SIZE // 2)
    query = rotate(
        query_raw.reshape(pieces_count, token_span, heads_query, HEAD_SIZE),
        cosine_table,
        sine_table,
    ).astype(jnp.bfloat16)
    key = rotate(
        key_unrotated.reshape(pieces_count, token_span, heads_key, HEAD_SIZE),
        cosine_table,
        sine_table,
    ).astype(jnp.bfloat16)
    value = value_projected.reshape(pieces_count, token_span, heads_key, HEAD_SIZE).astype(
        jnp.bfloat16
    )
    d_attended = cotangent.reshape(pieces_count, token_span, heads_query, HEAD_SIZE)
    attended, query_back, key_rotated_back, value_returned = jax.vmap(segment_pass)(
        query, key, value, d_attended
    )
    attended_flat = attended.reshape(segment_length, heads_query * HEAD_SIZE)
    d_query = (
        inverse_rotation(query_back, cosine_table, sine_table)
        .astype(jnp.bfloat16)
        .reshape(segment_length, heads_query * HEAD_SIZE)
    )
    key_gradient = (
        inverse_rotation(key_rotated_back, cosine_table, sine_table)
        .astype(jnp.bfloat16)
        .reshape(segment_length, heads_key * HEAD_SIZE)
    )
    value_gradient = value_returned.astype(jnp.bfloat16).reshape(
        segment_length, heads_key * HEAD_SIZE
    )
    back_query, back_key, back_value = (
        lax.all_gather(w_query, "dp", axis=0, tiled=True),
        lax.all_gather(key_weight, "dp", axis=0, tiled=True),
        lax.all_gather(value_weight, "dp", axis=0, tiled=True),
    )
    joined = jnp.concatenate([d_query, key_gradient, value_gradient], 1)
    block = gathered
    grads = lax.psum_scatter(
        lax.dot_general(block, joined, contract_first, preferred_element_type=jnp.float32).astype(
            jnp.bfloat16
        ),
        "dp",
        scatter_dimension=0,
        tiled=True,
    ).astype(jnp.float32)
    width_query = w_query.shape[1]
    width_key = key_weight.shape[1]
    grad_query = grads[:, :width_query]
    grad_key = grads[:, width_query : width_query + width_key]
    grad_value = grads[:, width_query + width_key :]
    total = jnp.zeros((tokens.shape[0] * lax.axis_size("tensor"), gathered.shape[1]), jnp.float32)
    for grad_part, weight in (
        (d_query, back_query),
        (key_gradient, back_key),
        (value_gradient, back_value),
    ):
        block = grad_part
        total = total + lax.dot_general(
            block, weight, contract_last, preferred_element_type=jnp.float32
        )
    d_normed = lax.psum_scatter(
        total.astype(jnp.bfloat16), "tensor", scatter_dimension=0, tiled=True
    ).astype(jnp.float32)
    pre_part = jnp.sum(d_normed * unit_one, 0)
    scaled_in = d_normed * pre_gain
    grad_tokens = (
        inv_one * (scaled_in - unit_one * jnp.mean(scaled_in * unit_one, -1, keepdims=True))
    ).astype(jnp.bfloat16)
    grad_pre = lax.psum(pre_part, ("dp", "tensor"))
    return (attended_flat, grad_tokens, grad_query, grad_key, grad_value, grad_pre)


F32 = jnp.float32
BF16 = jnp.bfloat16
NN = (((1,), (0,)), ((), ()))
NT = (((1,), (1,)), ((), ()))
TN = (((0,), (0,)), ((), ()))


def swap_halves(values):
    half = values.shape[-1] // 2
    return jnp.concatenate([values[:, half:], values[:, :half]], -1)


W_SLOT = (0, 1, 2, 2, 2, 3, 3, 2)


def whole_kernel(
    dims,
    tok_hbm,
    gain_hbm,
    wq_ref,
    wk_ref,
    wv_ref,
    cot_hbm,
    cos_hbm,
    sin_hbm,
    mask_hbm,
    att_ref,
    gtok_ref,
    gq_ref,
    gk_ref,
    gv_ref,
    gpre_ref,
    tok_ref,
    gain_ref,
    cot_ref,
    cos_ref,
    sin_ref,
    mask_ref,
    x,
    xt,
    w,
    wt,
    proj,
    dproj,
    g,
    pr,
    dr,
    ar,
    dn,
    rb,
    pb1,
    pb2,
    ws,
    wr,
    xs,
    xr,
    qr,
    ms,
    mr,
    gs,
    gr,
    zs,
    zr,
    ps,
    prs,
    ls,
    ins,
):
    n_dp, n_t, chunks, rep, hd, tile = dims
    dp = lax.axis_index("dp")
    t = lax.axis_index("tensor")
    rows = tok_ref.shape[0]
    width = tok_ref.shape[1]
    shard = wq_ref.shape[0]
    qw = rep * hd
    cw = qw + 2 * hd
    half = shard // 2
    n_chip = n_dp // 2
    parts = width // tile
    core = lax.rem(dp, 2)
    chip = lax.div(dp, 2)
    mate, px, py = dp ^ 1, dp ^ 2, dp ^ 4

    barrier = pltpu.get_barrier_semaphore()

    def greet(d, z):
        pl.semaphore_signal(
            barrier, inc=1, device_id=(d, z), device_id_type=pl.DeviceIdType.MESH
        )

    greet(px, t)
    greet(py, t)

    @pl.when(t < n_t - 1)
    def _():
        greet(dp, t + 1)

    @pl.when(t > 0)
    def _():
        greet(dp, t - 1)

    greet(mate, t)

    loads = [
        pltpu.make_async_copy(src, dst, ins.at[i])
        for i, (src, dst) in enumerate(
            (
                (tok_hbm, tok_ref),
                (gain_hbm, gain_ref),
                (cos_hbm, cos_ref),
                (sin_hbm, sin_ref),
                (mask_hbm, mask_ref),
                (cot_hbm, cot_ref),
            )
        )
    ]

    def own_copies(j):
        here = pl.ds(pl.multiple_of(dp * shard, 16), shard)
        return (
            pltpu.make_async_copy(
                wq_ref.at[:, j * qw : (j + 1) * qw], w.at[j, here, 0:qw], ls.at[j]
            ),
            pltpu.make_async_copy(
                wk_ref.at[:, j * hd : (j + 1) * hd], w.at[j, here, qw : qw + hd], ls.at[j]
            ),
            pltpu.make_async_copy(
                wv_ref.at[:, j * hd : (j + 1) * hd], w.at[j, here, qw + hd : cw], ls.at[j]
            ),
        )

    def own_wait(j):
        here = pl.ds(pl.multiple_of(dp * shard, 16), shard)
        pltpu.make_async_copy(wq_ref.at[:, 0:cw], w.at[j, here], ls.at[j]).wait()

    loads[0].start()
    loads[1].start()
    for j in range(chunks):
        for copy in own_copies(j):
            copy.start()
    for copy in loads[2:]:
        copy.start()

    def rdma(src, dst, ssem, rsem, d, z):
        return pltpu.make_async_remote_copy(
            src_ref=src,
            dst_ref=dst,
            send_sem=ssem,
            recv_sem=rsem,
            device_id=(d, z),
            device_id_type=pl.DeviceIdType.MESH,
        )

    def wrow(who, h=None):
        if h is None:
            return pl.ds(pl.multiple_of(who * shard, 16), shard)
        return pl.ds(pl.multiple_of(who * shard + h * half, 16), half)

    def wcopy(kind, j, origin, to, h=None):
        place = w.at[j, wrow(origin, h)]
        return rdma(place, place, ws.at[j], wr.at[W_SLOT[kind], j], to, t)

    def whole(count, j, slot):
        place = w.at[j, 0 : count * shard]
        return rdma(place, place, ws.at[j], wr.at[slot, j], mate, t)

    def offer(j):
        wcopy(0, j, dp, px).start()
        wcopy(1, j, dp, py).start()

    low = t < n_t // 2
    sign = jnp.where(low, 1, -1)
    m = jnp.where(low, t, n_t - 1 - t)
    fwd = jnp.where(low, 0, 1)
    piece, quarter = rows // 2, rows // 4
    mine_next = t + sign

    def xcopy(way, o, h, origin, to):
        place = x.at[pl.ds(pl.multiple_of(origin * rows + h * piece, piece), piece)]
        return rdma(place, place, xs.at[min(o, 1)], xr.at[way, o, h], dp, to)

    def xpart(origin, count, k):
        place = x.at[pl.ds(pl.multiple_of(origin * rows, rows), count)]
        return rdma(place, place, xs.at[k], qr.at[0], dp, mine_next)

    def qcopy(k, origin, to):
        first = pl.multiple_of(origin * rows + piece + k * quarter, quarter)
        place = x.at[pl.ds(first, quarter)]
        return rdma(place, place, xs.at[0], qr.at[0], dp, to)

    own_wait(0)
    pl.semaphore_wait(barrier, 3 + jnp.where(m == 0, 1, 2))
    offer(0)
    own_wait(1)
    offer(1)
    loads[0].wait()
    loads[1].wait()
    tokens = tok_ref[...].astype(F32)
    inv = lax.rsqrt(jnp.mean(tokens * tokens, -1, keepdims=True) + EPS)
    x[pl.ds(pl.multiple_of(t * rows, rows), rows), :] = (
        (tokens * inv) * gain_ref[...][None, :]
    ).astype(BF16)

    @pl.when(t < n_t - 1)
    def _():
        xcopy(0, 0, 0, t, t + 1).start()

    @pl.when(t > 0)
    def _():
        xcopy(1, 0, 0, t, t - 1).start()

    @pl.when(t < n_t - 2)
    def _():
        xcopy(0, 0, 1, t, t + 1).start()

    @pl.when(t > 1)
    def _():
        xcopy(1, 0, 1, t, t - 1).start()

    @pl.when(m > 0)
    def _():
        qcopy(0, t, t - sign).start()

    for j in range(2, chunks):
        own_wait(j)
    for j in range(chunks):
        wcopy(2, j, dp, mate).start()
    for copy in loads[2:]:
        copy.wait()

    def relay(j):
        wcopy(0, j, px, px).wait_recv()
        wcopy(5, j, px, py, h=0).start()
        wcopy(3, j, px, mate).start()
        wcopy(1, j, py, py).wait_recv()
        wcopy(6, j, py, px, h=1).start()
        wcopy(4, j, py, mate).start()

    def xrelay(o, h):
        split = o == 1 and h == 1
        above = (t - o >= 0) & (t < n_t - 1) if split else t - o >= 0
        below = (t + o < n_t) & (t > 0) if split else t + o < n_t

        @pl.when(above)
        def _():
            xcopy(0, o - 1, h, t - o, t).wait_recv()

            @pl.when(t + 1 < n_t)
            def _():
                xcopy(0, o, h, t - o, t + 1).start()

        @pl.when(below)
        def _():
            xcopy(1, o - 1, h, t + o, t).wait_recv()

            @pl.when(t > 0)
            def _():
                xcopy(1, o, h, t + o, t - 1).start()

    def xlate():
        @pl.when(m > 0)
        def _():
            qcopy(1, t, t - sign).start()

    def xfinish():
        @pl.when(m == 0)
        def _():
            xpart(t + sign, piece, 0).wait_recv()

    def far(j):
        whole(1, j, 3).wait_recv()
        wcopy(7, j, dp ^ 6, mate).start()

    def ready(j, relayed=False):
        if not relayed:
            far(j)
        whole(n_chip, j, 2).wait_recv()

    factor = query_scalar ** (-0.5)

    def mirror(b):
        return jnp.where(low, b, n_t - 1 - b)

    places = (
        t,
        jnp.where(m == 0, t + sign, t - sign),
        jnp.where(m == 0, t + 2 * sign, t + sign),
        mirror(n_t - 1),
    )

    def head_cols(j, i):
        return pl.ds(pl.multiple_of(j * qw + i * hd, hd), hd)

    def block_rows(b, count=1):
        return pl.ds(pl.multiple_of(b * rows, rows), count * rows)

    def tiles(*which):
        for slot, (j, p) in enumerate(which):
            here = block_rows(places[p])
            proj[slot] = lax.dot_general(x[here, :], w[j], NN, preferred_element_type=F32)
        for slot, (j, p) in enumerate(which):
            here = block_rows(places[p])
            cosv, sinv = cos_ref[...], sin_ref[...]

            def turn(v):
                return v * cosv + swap_halves(v) * sinv

            def unturn(v):
                return v * cosv - swap_halves(v) * sinv

            q = jnp.concatenate(
                [turn(proj[slot, :, i * hd : (i + 1) * hd]).astype(BF16) for i in range(rep)], 0
            )
            k = turn(proj[slot, :, qw : qw + hd]).astype(BF16)
            v = proj[slot, :, qw + hd : cw].astype(BF16)
            cot = jnp.concatenate(
                [cot_ref[here, head_cols(j, i)] for i in range(rep)], 0
            )
            bent = jnp.tanh(
                lax.dot_general(q, k, NT, preferred_element_type=F32) * factor / CAP
            )
            raised = jnp.exp(CAP * bent) * mask_ref[...]
            weights = raised / jnp.sum(raised, -1, keepdims=True)
            probs = weights.astype(BF16)
            att = lax.dot_general(probs, v, NN, preferred_element_type=F32).astype(BF16)
            d_probs = lax.dot_general(cot, v, NT, preferred_element_type=F32)
            d_capped = weights * (d_probs - jnp.sum(weights * d_probs, -1, keepdims=True))
            ds = (d_capped * (1.0 - bent * bent) * factor).astype(BF16)
            dq = lax.dot_general(ds, k, NN, preferred_element_type=F32)
            dk = lax.dot_general(ds, q, TN, preferred_element_type=F32)
            dv = lax.dot_general(probs, cot, TN, preferred_element_type=F32)
            for i in range(rep):
                part = slice(i * rows, (i + 1) * rows)
                att_ref[here, head_cols(j, i)] = att[part]
                dproj[j, here, i * hd : (i + 1) * hd] = unturn(dq[part]).astype(BF16)
            dproj[j, here, qw : qw + hd] = unturn(dk).astype(BF16)
            dproj[j, here, qw + hd : cw] = dv.astype(BF16)

    def flip_rows(p):
        here = block_rows(places[p])
        xt[:, here] = x[here, :].T

    def flip_weights(j):
        wt[j] = w[j].T

    def span(p):
        return pl.ds(pl.multiple_of(p * tile, tile), tile)

    def zcopy(way, b, p, to):
        return rdma(
            dn.at[block_rows(b), span(p)],
            rb.at[way, b, :, span(p)],
            zs.at[0],
            zr.at[way, b - 1 + way, p],
            dp,
            to,
        )

    def outward(b, p):
        zcopy(fwd, mirror(b), p, t + sign).start()

    def back(first, count, sent=None, begin=0, end=parts, flipped=chunks):
        here = block_rows(first, count)

        def cols(p, c2):
            total = jnp.zeros((count * rows, tile), F32)
            for j in range(flipped):
                total += lax.dot_general(
                    dproj[j, here, :], wt[j, :, span(p)], NN, preferred_element_type=F32
                )
            for j in range(flipped, chunks):
                total += lax.dot_general(
                    dproj[j, here, :], w[j, span(p), :], NT, preferred_element_type=F32
                )
            dn[here, span(p)] = total.astype(BF16)

            if sent is not None:

                @pl.when(m == 0)
                def _():
                    outward(sent, p)

            return c2

        lax.fori_loop(begin, end, cols, 0)

    strip = 64

    def gain_part(first, count, fresh):
        def cols(p, c2):
            def step(r, acc):
                here = pl.ds(pl.multiple_of(first * rows + r * strip, strip), strip)
                both = dn[here, span(p)].astype(F32) * x[here, span(p)].astype(F32)
                return acc + jnp.sum(both.reshape(strip // 8, 8, tile), 0)

            acc = lax.fori_loop(0, count * rows // strip, step, jnp.zeros((8, tile), F32))
            total = jnp.sum(acc, 0, keepdims=True)
            if not fresh:
                total = total + pb1[t, :, span(p)]
            pb1[t, :, span(p)] = total
            return c2

        lax.fori_loop(0, parts, cols, 0)

    lo, hi = pl.ds(0, half), pl.ds(half, half)

    def to_mate(j, i):
        return rdma(g.at[j, i, 0], pr.at[j, i], ms.at[j], mr.at[j, (i + 1) // 2], mate, t)

    def gcopy(kind, j, src, dst, to):
        return rdma(src, dst, gs.at[j], gr.at[min(kind // 2, 1), j], to, t)

    def d_x(j):
        return gcopy(0, j, pr.at[j, 0, lo], dr.at[j, lo], px)

    def d_y(j):
        return gcopy(1, j, pr.at[j, 0, hi], dr.at[j, hi], py)

    def x_lo(j):
        return gcopy(2, j, pr.at[j, 2, lo], ar.at[0, j, lo], px)

    def x_hi(j):
        return gcopy(3, j, pr.at[j, 2, hi], ar.at[0, j, hi], px)

    def y_lo(j):
        return gcopy(4, j, pr.at[j, 1, lo], ar.at[1, j, lo], py)

    def y_hi(j):
        return gcopy(5, j, pr.at[j, 1, hi], ar.at[1, j, hi], py)

    def add(*terms):
        total = terms[0].astype(F32)
        for term in terms[1:]:
            total = total + term.astype(F32)
        return total.astype(BF16)

    def product(j, first=0, last=n_chip):
        def share(i, c2):
            c = chip ^ (n_chip - 1 - i)
            for k, who in enumerate((2 * c + 1 - core, 2 * c + core)):
                here = pl.ds(pl.multiple_of(who * shard, 16), shard)
                g[j, i, k] = lax.dot_general(
                    xt[here, :], dproj[j], NN, preferred_element_type=F32
                ).astype(BF16)
                if k == 0:
                    to_mate(j, i).start()
            return c2

        lax.fori_loop(first, last, share, 0)

    def joined(j, i):
        to_mate(j, i).wait_recv()
        pr[j, i] = add(g[j, i, 1], pr[j, i])

    def on_chip_far(j):
        joined(j, 0)
        d_x(j).start()
        d_y(j).start()

    def on_chip_near(j):
        pair = pr.at[j, 1:3]
        rdma(pair, pair, ms.at[j], mr.at[j, 1], mate, t).wait_recv()
        pr[j, 1] = add(g[j, 1, 1], pr[j, 1])
        y_hi(j).start()
        pr[j, 2] = add(g[j, 2, 1], pr[j, 2])
        x_lo(j).start()

    def pass_on(j):
        gcopy(0, j, pr.at[j, 0], dr.at[j], px).wait_recv()
        pr[j, 1, lo] = add(pr[j, 1, lo], dr[j, lo])
        y_lo(j).start()
        pr[j, 2, hi] = add(pr[j, 2, hi], dr[j, hi])
        x_hi(j).start()

    def zsum(way, b, p):
        here = block_rows(b)
        cols = slice(p * tile, (p + 1) * tile)
        zcopy(way, b, p, t).wait_recv()
        dn[here, cols] = add(dn[here, cols], rb[way, b, :, cols])

    far_block = mirror(n_t - 1)
    rest = jnp.where(low, 0, 1)
    near_pair = jnp.where(low, 0, n_t - 2)

    def pass_far(p):
        @pl.when(m > 0)
        def _():
            zsum(fwd, far_block, p)
            outward(n_t - 1, p)

    def pass_inner(p):
        @pl.when(m > 0)
        def _():
            zsum(1 - fwd, mirror(0), p)
            zcopy(1 - fwd, mirror(0), p, t - sign).start()

    def pass_next(p):
        @pl.when(m > 0)
        def _():
            zsum(fwd, mirror(n_t - 2), p)
            outward(n_t - 2, p)

    def p1(o):
        return rdma(pb1.at[t], pb1.at[t], ps.at[0], prs.at[0], dp, t ^ o)

    def p2(o):
        return rdma(pb2.at[dp], pb2.at[dp], ps.at[1], prs.at[1], dp ^ o, t)

    def p1_all():
        place = pb1.at[0 : n_t - 1]
        return rdma(place, place, ps.at[0], prs.at[0], dp, mine_next)

    def p2_all():
        place = pb2.at[0 : n_dp - 1]
        return rdma(place, place, ps.at[1], prs.at[1], mate, t)

    def final(j):
        gcopy(2, j, pr.at[j, 0:2], ar.at[:, j], px).wait_recv()
        done = pr[j, 3].astype(F32) + ar[0, j].astype(F32) + ar[1, j].astype(F32)
        gq_ref[:, j * qw : (j + 1) * qw] = done[:, :qw]
        gk_ref[:, j * hd : (j + 1) * hd] = done[:, qw : qw + hd]
        gv_ref[:, j * hd : (j + 1) * hd] = done[:, qw + hd :]

    relay(0)
    offer(2)
    xrelay(1, 0)
    flip_rows(0)
    relay(1)
    offer(3)
    xrelay(1, 1)
    ready(0)
    tiles((0, 0))
    xrelay(2, 0)
    relay(2)
    flip_weights(0)
    far(1)
    xrelay(2, 1)
    xlate()
    ready(1, True)
    tiles((1, 0), (0, 2), (1, 2))
    flip_rows(2)
    relay(3)
    flip_weights(1)
    xrelay(3, 0)
    xrelay(3, 1)
    far(2)
    tiles((0, 3), (1, 3))
    flip_rows(3)
    ready(2, True)
    xfinish()
    far(3)
    tiles((0, 1), (2, 3))
    flip_rows(1)
    product(0, 0, 1)
    ready(3, True)
    tiles((3, 3))
    on_chip_far(0)
    back(far_block, 1, n_t - 1, 0, 1, 2)
    product(0, 1, 3)
    back(far_block, 1, n_t - 1, 1, 2, 2)
    on_chip_near(0)
    back(far_block, 1, n_t - 1, 2, parts, 2)
    gain_part(far_block, 1, True)
    tiles((1, 1))
    pass_on(0)
    product(1, 0, 3)
    pass_far(0)
    flip_weights(2)
    on_chip_far(1)
    flip_weights(3)
    tiles((2, 2), (3, 2))
    on_chip_near(1)
    back(mirror(n_t - 2), 1, n_t - 2, 0, parts - 1)
    back(mirror(n_t - 2), 1, None, parts - 1, parts)
    pass_far(1)
    tiles((2, 0), (2, 1))
    product(2, 0, 1)
    pass_on(1)
    tiles((3, 0), (3, 1))
    on_chip_far(2)
    pass_far(2)
    product(2, 1, 3)
    back(near_pair, 2)
    on_chip_near(2)
    gain_part(rest, n_t - 1, False)
    pb1[t] = pb1[t] / gain_ref[...][None, :]
    for o in range(1, n_t):
        p1(o).start()

    @pl.when(m == 0)
    def _():
        outward(n_t - 2, parts - 1)
        for p in range(parts):
            outward(1, p)

    product(3, 0, 3)
    pass_inner(0)
    on_chip_far(3)
    product(0, 3, 4)
    product(1, 3, 4)
    on_chip_near(3)
    pass_on(2)
    pass_inner(1)
    pass_next(0)
    product(2, 3, 4)
    product(3, 3, 4)
    pass_inner(2)
    pass_next(1)
    p1_all().wait_recv()
    total = pb1[0]
    for o in range(1, n_t):
        total = total + pb1[o]
    pb2[dp] = total
    for o in range(1, n_dp):
        p2(o).start()
    pass_next(2)
    for j in range(chunks):
        joined(j, 3)
    pass_on(3)
    for j in range(chunks):
        whole(n_dp - 1, j, 2).wait_send()
        rdma(g.at[j, :, 0], pr.at[j], ms.at[j], mr.at[j, 0], mate, t).wait_send()

    @pl.when(m == 0)
    def _():
        xpart(0, rows, 0).wait_send()
        rb[fwd, t] = jnp.zeros((rows, width), BF16)

    @pl.when(m > 0)
    def _():
        xpart(0, 2 * rows, 0).wait_send()
        xpart(0, (n_t - 1) * rows, 1).wait_send()

    p1_all().wait_send()
    for j in range(chunks - 1):
        final(j)
        gcopy(2, j, pr.at[j, 0:3], pr.at[j, 0:3], px).wait_send()

    mine = block_rows(t)
    tokens2 = tok_ref[...].astype(F32)
    inv2 = lax.rsqrt(jnp.mean(tokens2 * tokens2, -1, keepdims=True) + EPS)
    dots = jnp.zeros((rows, 1), F32)
    held = []
    for p in range(parts):
        cols = slice(p * tile, (p + 1) * tile)
        zcopy(1 - fwd, t, p, t).wait_recv()

        @pl.when(m > 0)
        def _():
            zcopy(fwd, t, p, t).wait_recv()

        d_normed = (
            dn[mine, cols].astype(F32) + rb[0, t, :, cols].astype(F32) + rb[1, t, :, cols].astype(F32)
        )
        unit = tok_ref[:, cols].astype(F32) * inv2
        e = d_normed * gain_ref[cols][None, :]
        dots = dots + jnp.sum(e * unit, -1, keepdims=True)
        held.append((cols, unit, e))
    mean = dots / width
    for cols, unit, e in held:
        gtok_ref[:, cols] = (inv2 * (e - unit * mean)).astype(BF16)
    p2_all().wait_recv()
    total = pb2[0]
    for o in range(1, n_dp):
        total = total + pb2[o]
    gpre_ref[...] = total[0]
    final(chunks - 1)

    p2_all().wait_send()
    gcopy(2, chunks - 1, pr.at[chunks - 1, 0:3], pr.at[chunks - 1, 0:3], px).wait_send()
    sent = dn.at[0 : (n_t - 1) * rows]
    rdma(sent, sent, zs.at[0], zr.at[0, 0, 0], dp, mine_next).wait_send()


def finish_kernel(*refs):
    count = len(refs) // 2
    sems = refs[-1]
    copies = [
        pltpu.make_async_copy(refs[i], refs[count + i], sems.at[i]) for i in range(count)
    ]
    for copy in copies:
        copy.start()
    for copy in copies:
        copy.wait()


def fused_per_device(tokens, cotangent, pre_gain, w_query, key_weight, value_weight):
    n_dp, n_t = lax.axis_size("dp"), lax.axis_size("tensor")
    rows, width = tokens.shape
    block = rows * n_t
    shard = w_query.shape[0]
    chunks = key_weight.shape[1] // HEAD_SIZE
    rep = w_query.shape[1] // key_weight.shape[1]
    qw = rep * HEAD_SIZE
    cw = qw + 2 * HEAD_SIZE
    kw = chunks * HEAD_SIZE
    half = HEAD_SIZE // 2
    parts = 3 if width % (3 * HEAD_SIZE) == 0 else 1
    n_chip = n_dp // 2
    place = np.arange(rows)
    freqs = BASE ** (-np.arange(half) / half)
    angles = (place % SEQ_LEN)[:, None] * freqs[None, :]
    cosine = np.concatenate([np.cos(angles)] * 2, -1).astype(np.float32)
    sine = np.concatenate([-np.sin(angles), np.sin(angles)], -1).astype(np.float32)
    mask = (place[None, :] <= place[:, None]) & (
        place[None, :] // SEQ_LEN == place[:, None] // SEQ_LEN
    )
    mask = np.tile(mask.astype(np.float32), (rep, 1))
    vmem = pl.BlockSpec(memory_space=pltpu.VMEM)
    hbm = pl.BlockSpec(memory_space=pl.ANY)
    dma = pltpu.SemaphoreType.DMA
    made = pl.pallas_call(
        functools.partial(whole_kernel, (n_dp, n_t, chunks, rep, HEAD_SIZE, width // parts)),
        out_shape=(
            pltpu.VMEM((block, chunks * qw), BF16),
            pltpu.VMEM((rows, width), BF16),
            pltpu.VMEM((shard, chunks * qw), F32),
            pltpu.VMEM((shard, kw), F32),
            pltpu.VMEM((shard, kw), F32),
            pltpu.VMEM((width,), F32),
        ),
        in_specs=[hbm] * 9,
        out_specs=(vmem,) * 6,
        scratch_shapes=[
            pltpu.VMEM((rows, width), BF16),
            pltpu.VMEM((width,), F32),
            pltpu.VMEM((block, chunks * qw), BF16),
            pltpu.VMEM(cosine.shape, F32),
            pltpu.VMEM(sine.shape, F32),
            pltpu.VMEM(mask.shape, F32),
            pltpu.VMEM((block, width), BF16),
            pltpu.VMEM((width, block), BF16),
            pltpu.VMEM((chunks, width, cw), BF16),
            pltpu.VMEM((chunks, cw, width), BF16),
            pltpu.VMEM((4, rows, cw), F32),
            pltpu.VMEM((chunks, block, cw), BF16),
            pltpu.VMEM((chunks, n_chip, 2, shard, cw), BF16),
            pltpu.VMEM((chunks, n_chip, shard, cw), BF16),
            pltpu.VMEM((chunks, shard, cw), BF16),
            pltpu.VMEM((2, chunks, shard, cw), BF16),
            pltpu.VMEM((block, width), BF16),
            pltpu.VMEM((2, n_t, rows, width), BF16),
            pltpu.VMEM((n_t, 1, width), F32),
            pltpu.VMEM((n_dp, 1, width), F32),
            dma((chunks,)),
            dma((4, chunks)),
            dma((2,)),
            dma((2, n_t - 1, 2)),
            dma((1,)),
            dma((chunks,)),
            dma((chunks, 3)),
            dma((chunks,)),
            dma((2, chunks)),
            dma((1,)),
            dma((2, n_t - 1, parts)),
            dma((2,)),
            dma((2,)),
            dma((chunks,)),
            dma((6,)),
        ],
        compiler_params=pltpu.CompilerParams(
            collective_id=0, has_side_effects=True, vmem_limit_bytes=57 * 1024 * 1024
        ),
    )(tokens, pre_gain, w_query, key_weight, value_weight, cotangent, cosine, sine, mask)
    return pl.pallas_call(
        finish_kernel,
        out_shape=(
            jax.ShapeDtypeStruct((block, chunks * qw), BF16),
            jax.ShapeDtypeStruct((rows, width), BF16),
            jax.ShapeDtypeStruct((shard, chunks * qw), F32),
            jax.ShapeDtypeStruct((shard, kw), F32),
            jax.ShapeDtypeStruct((shard, kw), F32),
            jax.ShapeDtypeStruct((width,), F32),
        ),
        in_specs=[vmem] * 6,
        out_specs=(hbm,) * 6,
        scratch_shapes=[
            dma((6,)),
        ],
        compiler_params=pltpu.CompilerParams(vmem_limit_bytes=16 * 1024 * 1024),
    )(*made)


def solution(mesh):
    fused = mesh.shape["dp"] == 8 and mesh.shape["tensor"] == 4
    placed = (
        P(("dp", "tensor"), None),
        P("dp", "tensor"),
        P(),
        P("dp", "tensor"),
        P("dp", "tensor"),
        P("dp", "tensor"),
    )
    return jax.shard_map(
        fused_per_device if fused else per_device,
        mesh=mesh,
        in_specs=placed,
        out_specs=(
            P("dp", "tensor"),
            P(("dp", "tensor"), None),
            P("dp", "tensor"),
            P("dp", "tensor"),
            P("dp", "tensor"),
            P(),
        ),
        check_vma=False,
    )
```
